512 devices in a mesh: gx: 8 (over z), gy: 64 (over x, y, core).
Axes of the slice: x: 4, y: 8, z: 8, core: 2. Of those that a mesh axis runs over, the one named last changes fastest.
Arguments:
- right_side: float32 [4194304], P(('gx', 'gy')), may hold values from -60 to 60
- reaction: float32 [4194304], P(('gx', 'gy')), may hold values from 0.5 to 2
- cell_slots: int32 [125, 65536], P(None, ('gx', 'gy')), may hold values from 0 to 12543
- cell_level: int32 [65536], P(('gx', 'gy')), may hold values from 0 to 2
- con_masters: int32 [5, 131072], P(None, ('gx', 'gy')), may hold values from 0 to 12287
- con_rows: int32 [131072], P(('gx', 'gy')), may hold values from 0 to 9
- send_lists: int32 [8, 262144], P(None, ('gx', 'gy')), may hold values from 0 to 8191
Outputs:
- solution: float32 [4194304], P(('gx', 'gy'))
- residual: float32 [4194304], P(('gx', 'gy'))
The draws below stay inside these ranges and needn't reach their ends.
Inputs may be any that keep to these rules, and one draw needn't show every extreme that they name: `cell_slots`: column block of rank d indexes d's local list: its 8192 owned unknowns, then 512 values from each of ranks d - 1, ..., d - 4, then from d + 1, ..., d + 4, then its 256 constrained values (rank d = 64 gx + gy). `cell_level`: A cell of level l has side 2^(-l). `con_masters`: slots among the same rank's owned and ghost values. `con_rows`: row of the interpolation table: 5 fine nodes on each half of a coarse edge. `send_lists`: row j of rank s lists s's owned unknowns that fill ghost block j of rank s + j + 1 (j < 4) or of rank s - (j - 3); rows without such a rank are unused.
All inputs are finite; a program needn't handle non-finite values.
Results may differ from the reference program's by a relative error of at most 0.0002.
Values sent between devices are 32-bit elements; how exact they have to be, the bound alone decides.
No kernel may reach another device: no remote copies, remote signals or barrier semaphores. Data moves between devices by JAX's collectives and lax.ppermute only.
A program may use at most 64 MiB of HBM per device.

```python
import math
import jax
import jax.numpy as jnp
import numpy as np
from jax import lax

NODES = 5
PEERS = 4
ITERS = 3
CELLS_DEV = 128
NOWN = 8192
GHOSTS = 512
NCON = 256
CELLS = 65536
NDOF = 4194304
NCON_ALL = 131072
LISTS = 262144
N_GX = 8
N_GY = 64


def draw_right_side(key, part):
    entries = NDOF
    position = jnp.arange(entries, dtype=jnp.float32) / entries
    rising = 1.0 + 2.0 * position
    first_key = jax.random.fold_in(jax.random.fold_in(key, 11), 0)
    normal_part = jnp.clip(jax.random.normal(first_key, (entries,), jnp.float32), -4.0, 4.0)
    return (normal_part * rising).astype(jnp.float32)


def set_ends(drawn, own_key, low, largest):
    extent = drawn.shape
    spot = [jax.random.randint(jax.random.fold_in(own_key, axis), (), 0, extent[axis]) for axis in range(len(extent))]
    drawn = drawn.at[tuple(spot)].set(low)
    longest = extent.index(max(extent))
    spot[longest] = (spot[longest] + 1) % extent[longest]
    return drawn.at[tuple(spot)].set(largest)


def block_levels(stream_key, shape, cuts, smallest, largest):
    def one(dim, shards_of):
        steps = jax.random.uniform(jax.random.fold_in(jax.random.fold_in(stream_key, 6), dim), (shards_of,), jnp.float32, smallest / len(cuts), largest / len(cuts))
        return jnp.repeat(jnp.exp(steps), shape[dim] // shards_of).reshape((-1,) + (1,) * (len(shape) - dim - 1))

    gain = one(*cuts[0])
    for cut in cuts[1:]:
        gain = gain * one(*cut)
    return gain


def setup_inputs(seed: int = 0) -> dict:
    key_list = jax.random.split(jax.random.key(seed), 8)
    return {
        "right_side": draw_right_side(jax.random.fold_in(key_list[7], 71), 0),
        "reaction": jnp.clip(jnp.exp(math.log(2.0) - 1.3862944 * jax.random.uniform(key_list[1], (NDOF,), jnp.float32) ** block_levels(key_list[1], (NDOF,), ((0, 512),), -0.2, 0.2)), 0.5, 2.0),
        "cell_slots": set_ends(jax.random.randint(key_list[2], (NODES ** 3, CELLS), 0, NOWN + 2 * PEERS * GHOSTS + NCON), jax.random.fold_in(key_list[2], 1), 0, (NOWN + 2 * PEERS * GHOSTS + NCON) - 1).astype(jnp.int32),
        "cell_level": set_ends(jax.random.randint(key_list[3], (CELLS,), 0, 3), jax.random.fold_in(key_list[3], 1), 0, 2).astype(jnp.int32),
        "con_masters": set_ends(jax.random.randint(key_list[4], (NODES, NCON_ALL), 0, NOWN + 2 * PEERS * GHOSTS), jax.random.fold_in(key_list[4], 1), 0, (NOWN + 2 * PEERS * GHOSTS) - 1).astype(jnp.int32),
        "con_rows": set_ends(jax.random.randint(key_list[5], (NCON_ALL,), 0, 10), jax.random.fold_in(key_list[5], 1), 0, 9).astype(jnp.int32),
        "send_lists": set_ends(jax.random.randint(key_list[6], (2 * PEERS, LISTS), 0, NOWN), jax.random.fold_in(key_list[6], 1), 0, NOWN - 1).astype(jnp.int32),
    }


def lagrange(node_list, points):
    node_count = len(node_list)
    values = np.ones((len(points), node_count))
    derivs = np.zeros((len(points), node_count))
    for basis_node in range(node_count):
        for other_node in range(node_count):
            if other_node != basis_node:
                values[:, basis_node] = values[:, basis_node] * (points - node_list[other_node]) / (node_list[basis_node] - node_list[other_node])
        for skipped in range(node_count):
            if skipped != basis_node:
                product_term = np.ones(len(points)) / (node_list[basis_node] - node_list[skipped])
                for other_node in range(node_count):
                    if other_node != basis_node and other_node != skipped:
                        product_term = product_term * (points - node_list[other_node]) / (node_list[basis_node] - node_list[other_node])
                derivs[:, basis_node] = derivs[:, basis_node] + product_term
    return (values, derivs)

def tables():
    gll_offset = np.sqrt(3.0 / 7.0)
    lobatto = np.array([0.0, (1.0 - gll_offset) / 2.0, 0.5, (1.0 + gll_offset) / 2.0, 1.0])
    inner_point = np.sqrt(5.0 - 2.0 * np.sqrt(10.0 / 7.0)) / 3.0
    outer_point = np.sqrt(5.0 + 2.0 * np.sqrt(10.0 / 7.0)) / 3.0
    inner_weight = (322.0 + 13.0 * np.sqrt(70.0)) / 900.0
    outer_weight = (322.0 - 13.0 * np.sqrt(70.0)) / 900.0
    points = np.array([-outer_point, -inner_point, 0.0, inner_point, outer_point])
    gauss_weights = np.array([outer_weight, inner_weight, 128.0 / 225.0, inner_weight, outer_weight])
    points = (points + 1.0) / 2.0
    gauss_weights = gauss_weights / 2.0
    shapes, slopes = lagrange(lobatto, points)
    fine_points = np.concatenate([lobatto / 2.0, (1.0 + lobatto) / 2.0])
    interp, unused_slopes = lagrange(lobatto, fine_points)
    quad_weights = np.kron(gauss_weights, np.kron(gauss_weights, gauss_weights))
    grad_x = np.kron(slopes, np.kron(shapes, shapes))
    grad_y = np.kron(shapes, np.kron(slopes, shapes))
    grad_z = np.kron(shapes, np.kron(shapes, slopes))
    stiffness = np.zeros((125, 125))
    for gradient in (grad_x, grad_y, grad_z):
        stiffness = stiffness + gradient.T @ (quad_weights[:, None] * gradient)
    return (jnp.asarray(interp, jnp.float32), jnp.asarray(stiffness, jnp.float32))

def cell_laplace(cell_values, cell_scale, stiffness):
    product = jnp.dot(stiffness, cell_values, precision=lax.Precision.HIGHEST, preferred_element_type=jnp.float32)
    return product * cell_scale[None, :]

def local_apply(own_values, ghosts, slot_map, cell_scale, masters, weights, stiffness):
    local_list = jnp.concatenate([own_values, ghosts.reshape(-1)])
    picked = local_list[masters]
    resolved = lax.optimization_barrier(jnp.sum(weights * picked, axis=0))
    full_list = jnp.concatenate([local_list, resolved])
    cell_values = full_list[slot_map]
    contrib = cell_laplace(cell_values, cell_scale, stiffness)
    summed = jnp.zeros(full_list.shape, jnp.float32).at[slot_map.reshape(-1)].add(contrib.reshape(-1))
    split_at = local_list.shape[0]
    spread = summed[:split_at].at[masters.reshape(-1)].add((weights * summed[split_at:][None, :]).reshape(-1))
    return spread

def reference(right_side, reaction, cell_slots, cell_level, con_masters, con_rows, send_lists):
    interp, stiffness = tables()
    rank_count = N_GX * N_GY
    block_count = 2 * PEERS
    offsets = [neighbour + 1 for neighbour in range(PEERS)] + [-(neighbour + 1) for neighbour in range(PEERS)]
    slot_maps = cell_slots.reshape(125, rank_count, CELLS_DEV).transpose(1, 0, 2)
    scales = jnp.exp2(-cell_level.astype(jnp.float32)).reshape(rank_count, CELLS_DEV)
    master_maps = con_masters.reshape(5, rank_count, NCON).transpose(1, 0, 2)
    selector = (con_rows.reshape(rank_count, NCON)[:, None, :] == jnp.arange(10, dtype=jnp.int32)[None, :, None]).astype(jnp.float32)
    weight_maps = jnp.einsum('tk,rtn->rkn', interp, selector, precision=lax.Precision.HIGHEST)
    list_rows = send_lists.reshape(block_count, rank_count, GHOSTS).transpose(1, 0, 2)
    rank_ids = jnp.arange(rank_count, dtype=jnp.int32)
    reactions = reaction.reshape(rank_count, NOWN)
    source_ids = [rank_ids - offset for offset in offsets]
    inside = [(source >= 0) & (source < rank_count) for source in source_ids]
    owner_ids = [jnp.clip(source, 0, rank_count - 1).astype(jnp.int32) for source in source_ids]

    def one_rank(packed):
        own_values, ghost_values, slot_map, cell_scale, masters, weights = packed
        return local_apply(own_values, ghost_values, slot_map, cell_scale, masters, weights, stiffness)

    def operate(vector):
        field_rows = vector.reshape(rank_count, NOWN)
        ghost_parts = []
        for neighbour in range(block_count):
            fetched = field_rows[owner_ids[neighbour][:, None], list_rows[owner_ids[neighbour], neighbour]]
            ghost_parts.append(jnp.where(inside[neighbour][:, None], fetched, 0.0))
        ghosts = jnp.stack(ghost_parts, axis=1)
        spread = lax.map(one_rank, (field_rows, ghosts, slot_maps, scales, master_maps, weight_maps))
        result = (spread[:, :NOWN] + reactions * field_rows).reshape(-1)
        returned = spread[:, NOWN:].reshape(rank_count, block_count, GHOSTS)
        for neighbour in range(block_count):
            target = owner_ids[neighbour][:, None] * NOWN + list_rows[owner_ids[neighbour], neighbour]
            addend = jnp.where(inside[neighbour][:, None], returned[:, neighbour], 0.0)
            result = result.at[target.reshape(-1)].add(addend.reshape(-1))
        return result
    solution = jnp.zeros_like(right_side)
    residual = right_side
    direction = right_side
    norm_now = jnp.sum(residual * residual)
    for iteration in range(ITERS):
        applied = operate(direction)
        step_size = norm_now / jnp.sum(direction * applied)
        solution = solution + step_size * direction
        residual = residual - step_size * applied
        norm_next = jnp.sum(residual * residual)
        direction = residual + norm_next / norm_now * direction
        norm_now = norm_next
    return (solution, residual)
```

```python
import jax
import jax.numpy as jnp
import numpy as np
from jax import lax
from jax.experimental import pallas as pl
from jax.experimental.pallas import tpu as pltpu
from jax.sharding import Mesh
from jax.sharding import PartitionSpec as P

F32 = jnp.float32
BF16 = jnp.bfloat16
I32 = jnp.int32
AXES = ("gx", "gy_0", "gy_1", "gy_2")
GROUP = ("gy_1", "gy_2")
REST = ("gx", "gy_0")
OFFSETS = (1, 2, 3, 4, -1, -2, -3, -4)
MEMBERS = 16
PARTS = 3
OWN_ROWS = 64
LOCAL_ROWS = 96
FULL_ROWS = 98
PAD_ROWS = 112


def lagrange(node_list, points):
    node_count = len(node_list)
    values = np.ones((len(points), node_count))
    derivs = np.zeros((len(points), node_count))
    for basis_node in range(node_count):
        for other_node in range(node_count):
            if other_node != basis_node:
                values[:, basis_node] = (
                    values[:, basis_node]
                    * (points - node_list[other_node])
                    / (node_list[basis_node] - node_list[other_node])
                )
        for skipped in range(node_count):
            if skipped != basis_node:
                product_term = np.ones(len(points)) / (node_list[basis_node] - node_list[skipped])
                for other_node in range(node_count):
                    if other_node != basis_node and other_node != skipped:
                        product_term = (
                            product_term
                            * (points - node_list[other_node])
                            / (node_list[basis_node] - node_list[other_node])
                        )
                derivs[:, basis_node] = derivs[:, basis_node] + product_term
    return (values, derivs)


def tables():
    gll_offset = np.sqrt(3.0 / 7.0)
    lobatto = np.array([0.0, (1.0 - gll_offset) / 2.0, 0.5, (1.0 + gll_offset) / 2.0, 1.0])
    inner_point = np.sqrt(5.0 - 2.0 * np.sqrt(10.0 / 7.0)) / 3.0
    outer_point = np.sqrt(5.0 + 2.0 * np.sqrt(10.0 / 7.0)) / 3.0
    inner_weight = (322.0 + 13.0 * np.sqrt(70.0)) / 900.0
    outer_weight = (322.0 - 13.0 * np.sqrt(70.0)) / 900.0
    points = np.array([-outer_point, -inner_point, 0.0, inner_point, outer_point])
    gauss_weights = np.array(
        [outer_weight, inner_weight, 128.0 / 225.0, inner_weight, outer_weight]
    )
    points = (points + 1.0) / 2.0
    gauss_weights = gauss_weights / 2.0
    shapes, slopes = lagrange(lobatto, points)
    fine_points = np.concatenate([lobatto / 2.0, (1.0 + lobatto) / 2.0])
    interp, unused_slopes = lagrange(lobatto, fine_points)
    quad_weights = np.kron(gauss_weights, np.kron(gauss_weights, gauss_weights))
    grad_x = np.kron(slopes, np.kron(shapes, shapes))
    grad_y = np.kron(shapes, np.kron(slopes, shapes))
    grad_z = np.kron(shapes, np.kron(shapes, slopes))
    stiffness = np.zeros((128, 128))
    for gradient in (grad_x, grad_y, grad_z):
        stiffness[:125, :125] += gradient.T @ (quad_weights[:, None] * gradient)
    interp_wide = np.zeros((8, 128))
    interp_wide[:5, :10] = interp.T
    return (jnp.asarray(interp_wide, F32), jnp.asarray(stiffness, F32))


def lane_pick(rows, lanes):
    return jnp.take_along_axis(rows, lanes, axis=1, mode="promise_in_bounds")


def pick(table, slots, first, last):
    row_of = lax.shift_right_logical(slots, 7)
    lane_of = lax.bitwise_and(slots, 127)
    picked = jnp.zeros(slots.shape, F32)
    for row in range(first, last):
        spread_row = jnp.broadcast_to(table[row : row + 1, :], slots.shape)
        picked = jnp.where(row_of == row, lane_pick(spread_row, lane_of), picked)
    return picked


def split(x):
    pieces = []
    for part in range(PARTS):
        piece = x.astype(BF16)
        pieces.append(piece)
        if part + 1 < PARTS:
            x = x - piece.astype(F32)
    return pieces


def scatter_add(total, slots, values, rows):
    count = slots.shape[1]
    row_of = lax.shift_right_logical(slots, 7).astype(F32).astype(BF16)
    lane_of = lax.bitwise_and(slots, 127).astype(F32).astype(BF16)
    row_ids = lax.broadcasted_iota(I32, (rows, count), 0).astype(F32).astype(BF16)
    lane_ids = lax.broadcasted_iota(I32, (128, count), 0).astype(F32).astype(BF16)
    row_hot = jnp.where(
        row_ids == jnp.broadcast_to(row_of, (rows, count)),
        jnp.ones((rows, count), BF16),
        jnp.zeros((rows, count), BF16),
    )
    lane_hot = lane_ids == jnp.broadcast_to(lane_of, (128, count))
    none = jnp.zeros((128, count), BF16)
    lane_values = jnp.concatenate(
        [
            jnp.where(lane_hot, jnp.broadcast_to(piece, (128, count)), none)
            for piece in split(values)
        ],
        axis=0,
    )
    return total + lax.dot_general(
        row_hot, lane_values, (((1,), (1,)), ((), ())), preferred_element_type=F32
    )


def folded(total):
    result = total[:, :128]
    for part in range(1, PARTS):
        result = result + total[:, 128 * part : 128 * part + 128]
    return result


def place_sends(place, sign, sends, pull):
    for member in range(MEMBERS):
        sends[member] = jnp.zeros(sends.shape[1:], F32)
    for block, offset in enumerate(OFFSETS):
        member = lax.bitwise_and(place + sign * offset, MEMBERS - 1)
        for quarter, row in enumerate(pull(block)):
            sends[member, quarter : quarter + 1, :] = row


def arrived(place, received, relayed, offset, quarter):
    position = place + offset
    member = lax.bitwise_and(position, MEMBERS - 1)
    outside = (position < 0) | (position >= MEMBERS)
    inner = received[member, quarter : quarter + 1, :]
    outer = relayed[lax.bitwise_and(member, 3), quarter : quarter + 1, :]
    return jnp.where(outside, outer, inner)


def pick_lists(place, vector, lists, sends):
    quarters = [
        pick(vector, lists[:, 128 * quarter : 128 * quarter + 128], 0, OWN_ROWS)
        for quarter in range(4)
    ]
    place_sends(
        place, 1, sends, lambda block: [quarter[block : block + 1, :] for quarter in quarters]
    )


def first_kernel(place_ref, vector, lists, sends):
    pick_lists(place_ref[0], vector, lists, sends)


def local_kernel(
    place_ref,
    vector,
    received,
    relayed,
    slots_in,
    level,
    masters_in,
    con_row,
    interp,
    stiffness,
    reaction,
    *rest,
):
    moments_of = rest[:-6]
    own, sends, table, slots, masters, cell_values = rest[-6:]
    place = place_ref[0]
    table[0:OWN_ROWS, :] = vector[...]
    for block, offset in enumerate(OFFSETS):
        for quarter in range(4):
            row = OWN_ROWS + 4 * block + quarter
            table[row : row + 1, :] = arrived(place, received, relayed, -offset, quarter)
    slots[120:128, :] = jnp.zeros((8, 128), I32)
    slots[0:125, :] = slots_in[...]
    masters[...] = jnp.zeros((8, 256), I32)
    masters[0:5, :] = masters_in[...]
    weights = []
    for half in range(2):
        lanes = slice(128 * half, 128 * half + 128)
        weight = lane_pick(interp[...], jnp.broadcast_to(con_row[:, lanes], (8, 128)))
        weights.append(weight)
        resolved = weight * pick(table, masters[:, lanes], 0, LOCAL_ROWS)
        table[LOCAL_ROWS + half : LOCAL_ROWS + half + 1, :] = jnp.sum(
            resolved, axis=0, keepdims=True
        )
    for group in range(16):
        cell_values[8 * group : 8 * group + 8, :] = pick(
            table, slots[8 * group : 8 * group + 8, :], 0, FULL_ROWS
        )
    products = jnp.dot(
        stiffness[...],
        cell_values[...],
        precision=lax.Precision.HIGHEST,
        preferred_element_type=F32,
    )
    products = products * jnp.exp2(-level[...].astype(F32))
    if moments_of:
        energy = jnp.sum(products * cell_values[...]) + jnp.sum(
            reaction[...] * vector[...] * vector[...]
        )
        vectors = [ref[...] for ref in moments_of] + [vector[...]]
        moments = [
            jnp.sum(vectors[degree // 2] * vectors[(degree + 1) // 2]) for degree in range(5)
        ] + [energy]
    cell_values[...] = products

    def cell_rows(step, total):
        base = pl.multiple_of(8 * step, 8)
        at = slots[pl.ds(base, 8), :]
        add = cell_values[pl.ds(base, 8), :]
        for row in range(0, 8, 2):
            total = scatter_add(
                total,
                jnp.concatenate([at[row : row + 1], at[row + 1 : row + 2]], axis=1),
                jnp.concatenate([add[row : row + 1], add[row + 1 : row + 2]], axis=1),
                PAD_ROWS,
            )
        return total

    summed = folded(
        lax.fori_loop(0, 16, cell_rows, jnp.zeros((PAD_ROWS, 128 * PARTS), F32))
    )
    total = jnp.zeros((PAD_ROWS, 128 * PARTS), F32)
    back = [
        weights[half]
        * jnp.broadcast_to(summed[LOCAL_ROWS + half : LOCAL_ROWS + half + 1, :], (8, 128))
        for half in range(2)
    ]
    for node in range(5):
        total = scatter_add(
            total,
            masters[node : node + 1, :],
            jnp.concatenate([part[node : node + 1, :] for part in back], axis=1),
            PAD_ROWS,
        )
    spread = summed + folded(total)
    own[...] = spread[0:OWN_ROWS, :] + reaction[...] * vector[...]

    def ghost_rows(block):
        first = OWN_ROWS + 4 * block
        return [spread[first + quarter : first + quarter + 1, :] for quarter in range(4)]

    place_sends(place, -1, sends, ghost_rows)
    if moments_of:
        lane = lax.broadcasted_iota(I32, (1, 128), 1)
        packed = jnp.zeros((1, 128), F32)
        for degree, moment in enumerate(moments):
            packed = jnp.where(lane == degree, moment, packed)
        for member in range(MEMBERS):
            sends[member, 4:5, :] = packed


def owner_kernel(place_ref, own, received, relayed, lists, vector, *sends):
    place = place_ref[0]
    total = jnp.zeros((OWN_ROWS, 128 * PARTS), F32)
    for block, offset in enumerate(OFFSETS):
        for half in range(2):
            lanes = slice(256 * half, 256 * half + 256)
            total = scatter_add(
                total,
                lists[block : block + 1, lanes],
                jnp.concatenate(
                    [
                        arrived(place, received, relayed, offset, 2 * half + quarter)
                        for quarter in range(2)
                    ],
                    axis=1,
                ),
                OWN_ROWS,
            )
    vector[...] = own[...] + folded(total)
    if sends:
        pick_lists(place, vector, lists, sends[0])


def last_kernel(moments_in, *refs):
    v = [ref[...] for ref in refs[:4]]
    solution, residual = refs[4:]
    sums = jnp.sum(moments_in[...], axis=0, keepdims=True)
    lane = lax.broadcasted_iota(I32, (1, 128), 1)
    mu = [
        jnp.sum(jnp.where(lane == degree, sums, 0.0), axis=1, keepdims=True)
        for degree in range(6)
    ]
    zero = jnp.zeros((1, 1), F32)
    one = jnp.ones((1, 1), F32)

    def form(p, q, shift):
        value = zero
        for i, left in enumerate(p):
            for k, right in enumerate(q):
                value = value + left * right * mu[i + k + shift]
        return value

    res = [one]
    direction = [one]
    sol = [zero]
    rr = mu[0]
    for iteration in range(3):
        step = rr / form(direction, direction, 1)
        applied = [zero] + direction
        sol = [
            (sol[i] if i < len(sol) else zero) + step * direction[i]
            for i in range(len(direction))
        ]
        res = [
            (res[i] if i < len(res) else zero) - step * applied[i] for i in range(len(applied))
        ]
        if iteration < 2:
            rr_next = form(res, res, 0)
            ratio = rr_next / rr
            direction = [
                res[i] + (ratio * direction[i] if i < len(direction) else zero)
                for i in range(len(res))
            ]
            rr = rr_next
    solution[...] = sol[0] * v[0] + sol[1] * v[1] + sol[2] * v[2]
    residual[...] = res[0] * v[0] + res[1] * v[1] + res[2] * v[2] + res[3] * v[3]


def relay_pairs():
    pairs = []
    for group in range(32):
        for member in range(4):
            if group + 1 < 32:
                source = MEMBERS * group + member
                pairs.append((source, source + MEMBERS))
            if group > 0:
                source = MEMBERS * group + 12 + member
                pairs.append((source, source - MEMBERS))
    return pairs


def on_device(right_side, reaction, cell_slots, cell_level, con_masters, con_rows, send_lists):
    interp, stiffness = tables()
    place = lax.axis_index(GROUP).astype(I32)
    place_ref = place.reshape(1)
    whole = pl.BlockSpec(memory_space=pltpu.VMEM)
    scalar = pl.BlockSpec(memory_space=pltpu.SMEM)
    tile = jax.ShapeDtypeStruct((OWN_ROWS, 128), F32)
    sends = jax.ShapeDtypeStruct((MEMBERS, 4, 128), F32)
    sends_wide = jax.ShapeDtypeStruct((MEMBERS, 8, 128), F32)
    vector = right_side.reshape(OWN_ROWS, 128)
    reaction = reaction.reshape(OWN_ROWS, 128)
    level = cell_level.reshape(1, 128)
    con_row = con_rows.reshape(1, 256)
    pairs = relay_pairs()

    def exchange(packed):
        received = lax.all_to_all(packed, GROUP, 0, 0)
        first = jnp.where(place < 4, 12, 0)
        relay = lax.dynamic_slice(received, (first, 0, 0), (4, 4, 128))
        return received, lax.ppermute(relay, AXES, pairs)

    packed = pl.pallas_call(
        first_kernel,
        out_shape=sends,
        in_specs=[scalar, whole, whole],
        out_specs=whole,
        name="first_lists",
    )(place_ref, vector, send_lists)
    vectors = [vector]
    for step in range(3):
        received, relayed = exchange(packed)
        last = step == 2
        extra = vectors[:2] if last else []
        own, packed = pl.pallas_call(
            local_kernel,
            out_shape=(tile, sends_wide if last else sends),
            in_specs=[scalar] + [whole] * (10 + len(extra)),
            out_specs=(whole, whole),
            scratch_shapes=[
                pltpu.VMEM((104, 128), F32),
                pltpu.VMEM((128, 128), I32),
                pltpu.VMEM((8, 256), I32),
                pltpu.VMEM((128, 128), F32),
            ],
            name="local_apply",
        )(
            place_ref,
            vectors[-1],
            received,
            relayed,
            cell_slots,
            level,
            con_masters,
            con_row,
            interp,
            stiffness,
            reaction,
            *extra,
        )
        received, relayed = exchange(packed)
        if last:
            group_sums = jnp.sum(received[:, 4, :], axis=0)
            moments = lax.all_to_all(
                jnp.broadcast_to(group_sums[None], (32, 128)), REST, 0, 0
            )
        outs = pl.pallas_call(
            owner_kernel,
            out_shape=(tile,) if last else (tile, sends),
            in_specs=[scalar] + [whole] * 4,
            out_specs=(whole,) if last else (whole, whole),
            name="owner_sum",
        )(place_ref, own, received, relayed, send_lists)
        vectors.append(outs[0])
        if not last:
            packed = outs[1]
    solution_rows, residual_rows = pl.pallas_call(
        last_kernel,
        out_shape=(tile, tile),
        in_specs=[whole] * 5,
        out_specs=(whole, whole),
        name="combine",
    )(moments, *vectors)
    return (solution_rows.reshape(-1), residual_rows.reshape(-1))


def solution(mesh):
    torus = Mesh(mesh.devices.reshape(mesh.shape["gx"], 4, 8, 2), AXES)
    placed = (
        P(AXES),
        P(AXES),
        P(None, AXES),
        P(AXES),
        P(None, AXES),
        P(AXES),
        P(None, AXES),
    )
    return jax.shard_map(
        on_device, mesh=torus, in_specs=placed, out_specs=(P(AXES), P(AXES)), check_vma=False
    )
```

```python
import jax
import jax.numpy as jnp
import numpy as np
from jax import lax
from jax.experimental import pallas as pl
from jax.experimental.pallas import tpu as pltpu
from jax.sharding import Mesh
from jax.sharding import PartitionSpec as P

F32 = jnp.float32
BF16 = jnp.bfloat16
I32 = jnp.int32
AXES = ("gx", "gy_0", "gy_1", "gy_2")
GROUP = ("gy_1", "gy_2")
REST = ("gx", "gy_0")
OFFSETS = (1, 2, 3, 4, -1, -2, -3, -4)
MEMBERS = 16
PARTS = 3
OWN_ROWS = 64
LOCAL_ROWS = 96
FULL_ROWS = 98
GHOST_ROWS = 48


def lagrange(node_list, points):
    node_count = len(node_list)
    values = np.ones((len(points), node_count))
    derivs = np.zeros((len(points), node_count))
    for basis_node in range(node_count):
        for other_node in range(node_count):
            if other_node != basis_node:
                values[:, basis_node] = (
                    values[:, basis_node]
                    * (points - node_list[other_node])
                    / (node_list[basis_node] - node_list[other_node])
                )
        for skipped in range(node_count):
            if skipped != basis_node:
                product_term = np.ones(len(points)) / (node_list[basis_node] - node_list[skipped])
                for other_node in range(node_count):
                    if other_node != basis_node and other_node != skipped:
                        product_term = (
                            product_term
                            * (points - node_list[other_node])
                            / (node_list[basis_node] - node_list[other_node])
                        )
                derivs[:, basis_node] = derivs[:, basis_node] + product_term
    return (values, derivs)


def tables():
    gll_offset = np.sqrt(3.0 / 7.0)
    lobatto = np.array([0.0, (1.0 - gll_offset) / 2.0, 0.5, (1.0 + gll_offset) / 2.0, 1.0])
    inner_point = np.sqrt(5.0 - 2.0 * np.sqrt(10.0 / 7.0)) / 3.0
    outer_point = np.sqrt(5.0 + 2.0 * np.sqrt(10.0 / 7.0)) / 3.0
    inner_weight = (322.0 + 13.0 * np.sqrt(70.0)) / 900.0
    outer_weight = (322.0 - 13.0 * np.sqrt(70.0)) / 900.0
    points = np.array([-outer_point, -inner_point, 0.0, inner_point, outer_point])
    gauss_weights = np.array(
        [outer_weight, inner_weight, 128.0 / 225.0, inner_weight, outer_weight]
    )
    points = (points + 1.0) / 2.0
    gauss_weights = gauss_weights / 2.0
    shapes, slopes = lagrange(lobatto, points)
    fine_points = np.concatenate([lobatto / 2.0, (1.0 + lobatto) / 2.0])
    interp, _ = lagrange(lobatto, fine_points)
    quad_weights = np.kron(gauss_weights, np.kron(gauss_weights, gauss_weights))
    grad_x = np.kron(slopes, np.kron(shapes, shapes))
    grad_y = np.kron(shapes, np.kron(slopes, shapes))
    grad_z = np.kron(shapes, np.kron(shapes, slopes))
    stiffness = np.zeros((128, 128))
    for gradient in (grad_x, grad_y, grad_z):
        stiffness[:125, :125] += gradient.T @ (quad_weights[:, None] * gradient)
    interp_wide = np.zeros((8, 128))
    interp_wide[:5, :10] = interp.T
    return (jnp.asarray(interp_wide, F32), jnp.asarray(stiffness, F32))


def lane_pick(rows, lanes):
    return jnp.take_along_axis(rows, lanes, axis=1, mode="promise_in_bounds")


def pick(table, slots, first, last, picked=None):
    row_of = lax.shift_right_logical(slots, 7)
    lane_of = lax.bitwise_and(slots, 127)
    if picked is None:
        picked = jnp.zeros(slots.shape, F32)
    for row in range(first, last):
        spread_row = jnp.broadcast_to(table[row : row + 1, :], slots.shape)
        picked = jnp.where(row_of == row, lane_pick(spread_row, lane_of), picked)
    return picked


def split(x):
    pieces = []
    for part in range(PARTS):
        piece = x.astype(BF16)
        pieces.append(piece)
        if part + 1 < PARTS:
            x = x - piece.astype(F32)
    return pieces


def scatter(entries, first, rows):
    row_ids = lax.broadcasted_iota(I32, (rows, 128), 0).astype(F32).astype(BF16)
    lane_ids = lax.broadcasted_iota(I32, (128, 128), 0).astype(F32).astype(BF16)
    none = jnp.zeros((rows, 128), BF16)
    total = None
    for start in range(0, len(entries), 16):
        row_values = []
        lane_hots = []
        for slots, values in entries[start : start + 16]:
            row_of = (lax.shift_right_logical(slots, 7) - first).astype(F32).astype(BF16)
            lane_of = lax.bitwise_and(slots, 127).astype(F32).astype(BF16)
            row_hot = row_ids == jnp.broadcast_to(row_of, (rows, 128))
            lane_hot = lane_ids == jnp.broadcast_to(lane_of, (128, 128))
            row_values.append(
                jnp.concatenate(
                    [
                        jnp.where(row_hot, jnp.broadcast_to(piece, (rows, 128)), none)
                        for piece in split(values)
                    ],
                    axis=0,
                )
            )
            lane_hots.append(
                jnp.where(lane_hot, jnp.ones((128, 128), BF16), jnp.zeros((128, 128), BF16))
            )
        part = lax.dot_general(
            jnp.concatenate(row_values, axis=1),
            jnp.concatenate(lane_hots, axis=1),
            (((1,), (1,)), ((), ())),
            preferred_element_type=F32,
        )
        total = part if total is None else total + part
    result = total[:rows, :]
    for part in range(1, PARTS):
        result = result + total[rows * part : rows * part + rows, :]
    return result


def place_sends(place, sign, sends, pull):
    for member in range(MEMBERS):
        sends[member] = jnp.zeros(sends.shape[1:], F32)
    for block, offset in enumerate(OFFSETS):
        position = place + sign * offset
        outside = (position < 0) | (position >= MEMBERS)
        member = lax.bitwise_xor(
            lax.bitwise_and(position, MEMBERS - 1), jnp.where(outside, 1, 0)
        )
        for quarter, row in enumerate(pull(block)):
            sends[member, quarter : quarter + 1, :] = row


def arrived(place, received, relayed, offset, quarter):
    position = place + offset
    member = lax.bitwise_and(position, MEMBERS - 1)
    outside = (position < 0) | (position >= MEMBERS)
    inner = received[member, quarter : quarter + 1, :]
    outer = relayed[lax.bitwise_and(member, 3), quarter : quarter + 1, :]
    return jnp.where(outside, outer, inner)


def pick_lists(place, vector, lists, sends):
    quarters = [
        pick(vector, lists[:, 128 * quarter : 128 * quarter + 128], 0, OWN_ROWS)
        for quarter in range(4)
    ]
    place_sends(
        place, 1, sends, lambda block: [quarter[block : block + 1, :] for quarter in quarters]
    )


def first_kernel(place_ref, vector, lists, sends):
    pick_lists(place_ref[0], vector, lists, sends)


def near_kernel(vector, slots_in, masters_in, cell_part, master_part, slots, masters):
    slots[120:128, :] = jnp.zeros((8, 128), I32)
    slots[0:125, :] = slots_in[...]
    masters[...] = jnp.zeros((8, 256), I32)
    masters[0:5, :] = masters_in[...]
    for half in range(2):
        lanes = slice(128 * half, 128 * half + 128)
        master_part[:, lanes] = pick(vector, masters[:, lanes], 0, OWN_ROWS)
    for group in range(16):
        group_rows = slice(8 * group, 8 * group + 8)
        cell_part[group_rows, :] = pick(vector, slots[group_rows, :], 0, OWN_ROWS)


def con_weights(con_row, interp):
    return [
        lane_pick(
            interp[...],
            jnp.broadcast_to(con_row[:, 128 * half : 128 * half + 128], (8, 128)),
        )
        for half in range(2)
    ]


def cell_products(
    place,
    received,
    relayed,
    cell_part,
    master_part,
    slots,
    level,
    masters,
    con_row,
    interp,
    stiffness,
    table,
    cell_values,
    products,
):
    for block, offset in enumerate(OFFSETS):
        for quarter in range(4):
            row = OWN_ROWS + 4 * block + quarter
            table[row : row + 1, :] = arrived(place, received, relayed, -offset, quarter)
    for half, weight in enumerate(con_weights(con_row, interp)):
        lanes = slice(128 * half, 128 * half + 128)
        resolved = weight * pick(
            table, masters[:, lanes], OWN_ROWS, LOCAL_ROWS, master_part[:, lanes]
        )
        table[LOCAL_ROWS + half : LOCAL_ROWS + half + 1, :] = jnp.sum(
            resolved, axis=0, keepdims=True
        )
    for group in range(16):
        group_rows = slice(8 * group, 8 * group + 8)
        cell_values[group_rows, :] = pick(
            table, slots[group_rows, :], OWN_ROWS, FULL_ROWS, cell_part[group_rows, :]
        )
    products[...] = jnp.dot(
        stiffness[...],
        cell_values[...],
        precision=lax.Precision.HIGHEST,
        preferred_element_type=F32,
    ) * jnp.exp2(-level[...].astype(F32))


def cell_entries(slots, products):
    return [(slots[row : row + 1, :], products[row : row + 1, :]) for row in range(125)]


def con_entries(masters, back):
    return [
        (
            masters[node : node + 1, 128 * half : 128 * half + 128],
            back[node : node + 1, 128 * half : 128 * half + 128],
        )
        for node in range(5)
        for half in range(2)
    ]


def ghost_sums(place, slots, masters, con_row, interp, products, sends, back):
    spread = scatter(cell_entries(slots, products), OWN_ROWS, GHOST_ROWS)
    con_first = LOCAL_ROWS - OWN_ROWS
    for half, weight in enumerate(con_weights(con_row, interp)):
        sums = spread[con_first + half : con_first + half + 1, :]
        back[:, 128 * half : 128 * half + 128] = weight * jnp.broadcast_to(sums, (8, 128))
    spread = spread + scatter(con_entries(masters, back), OWN_ROWS, GHOST_ROWS)
    place_sends(
        place,
        -1,
        sends,
        lambda block: [spread[row : row + 1, :] for row in range(4 * block, 4 * block + 4)],
    )


def local_kernel(
    place_ref,
    received,
    relayed,
    cell_part,
    master_part,
    slots,
    level,
    masters,
    con_row,
    interp,
    stiffness,
    products,
    sends,
    back,
    table,
    cell_values,
):
    place = place_ref[0]
    cell_products(
        place,
        received,
        relayed,
        cell_part,
        master_part,
        slots,
        level,
        masters,
        con_row,
        interp,
        stiffness,
        table,
        cell_values,
        products,
    )
    ghost_sums(place, slots, masters, con_row, interp, products, sends, back)


def last_local_kernel(
    place_ref,
    received,
    relayed,
    cell_part,
    master_part,
    slots,
    level,
    masters,
    con_row,
    interp,
    stiffness,
    reaction,
    first,
    second,
    third,
    products,
    sends,
    back,
    table,
    cell_values,
):
    local_kernel(
        place_ref,
        received,
        relayed,
        cell_part,
        master_part,
        slots,
        level,
        masters,
        con_row,
        interp,
        stiffness,
        products,
        sends,
        back,
        table,
        cell_values,
    )
    vectors = [ref[...] for ref in (first, second, third)]
    sums = [jnp.sum(vectors[degree // 2] * vectors[(degree + 1) // 2]) for degree in range(5)]
    sums.append(
        jnp.sum(products[...] * cell_values[...])
        + jnp.sum(reaction[...] * vectors[2] * vectors[2])
    )
    lane = lax.broadcasted_iota(I32, (1, 128), 1)
    packed = jnp.zeros((1, 128), F32)
    for degree, value in enumerate(sums):
        packed = jnp.where(lane == degree, value, packed)
    for member in range(MEMBERS):
        sends[member, 4:5, :] = packed


def own_kernel(slots, masters, products, back, reaction, vector, own):
    spread = scatter(cell_entries(slots, products) + con_entries(masters, back), 0, OWN_ROWS)
    own[...] = spread + reaction[...] * vector[...]


def owner_sum(place, own, received, relayed, lists, vector):
    entries = [
        (
            lists[block : block + 1, 128 * quarter : 128 * quarter + 128],
            arrived(place, received, relayed, offset, quarter),
        )
        for block, offset in enumerate(OFFSETS)
        for quarter in range(4)
    ]
    vector[...] = own[...] + scatter(entries, 0, OWN_ROWS)


def owner_kernel(place_ref, own, received, relayed, lists, vector, sends):
    place = place_ref[0]
    owner_sum(place, own, received, relayed, lists, vector)
    pick_lists(place, vector, lists, sends)


def final_owner_kernel(place_ref, own, received, relayed, lists, vector):
    owner_sum(place_ref[0], own, received, relayed, lists, vector)


def last_kernel(moments, first, second, third, fourth, solution, residual):
    v = [ref[...] for ref in (first, second, third, fourth)]
    sums = moments[0]
    for member in range(1, moments.shape[0]):
        sums = sums + moments[member]
    lane = lax.broadcasted_iota(I32, (1, 128), 1)
    mu = [
        jnp.sum(jnp.where(lane == degree, sums, 0.0), axis=1, keepdims=True)
        for degree in range(6)
    ]
    zero = jnp.zeros((1, 1), F32)
    one = jnp.ones((1, 1), F32)

    def form(p, q, shift):
        value = zero
        for i, left in enumerate(p):
            for k, right in enumerate(q):
                value = value + left * right * mu[i + k + shift]
        return value

    res = [one]
    direction = [one]
    sol = [zero]
    rr = mu[0]
    for iteration in range(3):
        step = rr / form(direction, direction, 1)
        applied = [zero] + direction
        sol = [
            (sol[i] if i < len(sol) else zero) + step * direction[i]
            for i in range(len(direction))
        ]
        res = [
            (res[i] if i < len(res) else zero) - step * applied[i] for i in range(len(applied))
        ]
        if iteration < 2:
            rr_next = form(res, res, 0)
            ratio = rr_next / rr
            direction = [
                res[i] + (ratio * direction[i] if i < len(direction) else zero)
                for i in range(len(res))
            ]
            rr = rr_next
    solution[...] = sol[0] * v[0] + sol[1] * v[1] + sol[2] * v[2]
    residual[...] = res[0] * v[0] + res[1] * v[1] + res[2] * v[2] + res[3] * v[3]


def relay_pairs():
    pairs = []
    for group in range(32):
        for member in range(4):
            if group + 1 < 32:
                source = MEMBERS * group + member
                pairs.append((source, (source + MEMBERS) ^ 1))
            if group > 0:
                source = MEMBERS * group + 12 + member
                pairs.append((source, (source - MEMBERS) ^ 1))
    return pairs


def on_device(right_side, reaction, cell_slots, cell_level, con_masters, con_rows, send_lists):
    interp, stiffness = tables()
    place = lax.axis_index(GROUP).astype(I32)
    place_ref = place.reshape(1)
    whole = pl.BlockSpec(memory_space=pltpu.VMEM)
    scalar = pl.BlockSpec(memory_space=pltpu.SMEM)
    tile = jax.ShapeDtypeStruct((OWN_ROWS, 128), F32)
    sends = jax.ShapeDtypeStruct((MEMBERS, 4, 128), F32)
    vector = right_side.reshape(OWN_ROWS, 128)
    reaction = reaction.reshape(OWN_ROWS, 128)
    level = cell_level.reshape(1, 128)
    con_row = con_rows.reshape(1, 256)
    pairs = relay_pairs()

    def relay(received):
        first = jnp.where(place < 4, 12, 0)
        rows = lax.dynamic_slice(received, (first, 0, 0), (4, 4, 128))
        return lax.ppermute(rows, AXES, pairs)

    def kernel(body, outs, operands, scratch=()):
        return pl.pallas_call(
            body,
            out_shape=outs,
            in_specs=[scalar if operand is place_ref else whole for operand in operands],
            out_specs=jax.tree.map(lambda out: whole, outs),
            scratch_shapes=scratch,
        )(*operands)

    padded = jax.ShapeDtypeStruct((128, 128), F32)
    con_padded = jax.ShapeDtypeStruct((8, 256), F32)
    work = [pltpu.VMEM((104, 128), F32), pltpu.VMEM((128, 128), F32)]
    packed = kernel(first_kernel, sends, (place_ref, vector, send_lists))
    vectors = [vector]
    for step in range(3):
        vector = vectors[-1]
        received = lax.all_to_all(packed, GROUP, 0, 0)
        cell_part, master_part, slots, masters = kernel(
            near_kernel,
            (
                padded,
                con_padded,
                jax.ShapeDtypeStruct((128, 128), I32),
                jax.ShapeDtypeStruct((8, 256), I32),
            ),
            (vector, cell_slots, con_masters),
        )
        relayed = relay(received)
        operands = (
            place_ref,
            received,
            relayed,
            cell_part,
            master_part,
            slots,
            level,
            masters,
            con_row,
            interp,
            stiffness,
        )
        if step < 2:
            products, packed, back = kernel(
                local_kernel, (padded, sends, con_padded), operands, work
            )
        else:
            products, packed, back = kernel(
                last_local_kernel,
                (padded, jax.ShapeDtypeStruct((MEMBERS, 8, 128), F32), con_padded),
                operands + (reaction,) + tuple(vectors),
                work,
            )
        received = lax.all_to_all(packed, GROUP, 0, 0)
        own = kernel(own_kernel, tile, (slots, masters, products, back, reaction, vector))
        relayed = relay(received)
        if step < 2:
            vector, packed = kernel(
                owner_kernel, (tile, sends), (place_ref, own, received, relayed, send_lists)
            )
            vectors.append(vector)
        else:
            sums = jnp.broadcast_to(jnp.sum(received[:, 4:5, :], axis=0)[None], (32, 1, 128))
            moments = lax.all_to_all(sums, REST, 0, 0)
            vector = kernel(
                final_owner_kernel, tile, (place_ref, own, received, relayed, send_lists)
            )
            vectors.append(vector)
    solution_rows, residual_rows = kernel(last_kernel, (tile, tile), (moments, *vectors))
    return (solution_rows.reshape(-1), residual_rows.reshape(-1))


def solution(mesh):
    torus = Mesh(mesh.devices.reshape(mesh.shape["gx"], 4, 8, 2), AXES)
    placed = (
        P(AXES),
        P(AXES),
        P(None, AXES),
        P(AXES),
        P(None, AXES),
        P(AXES),
        P(None, AXES),
    )
    return jax.shard_map(
        on_device, mesh=torus, in_specs=placed, out_specs=(P(AXES), P(AXES)), check_vma=False
    )
```

```python
import jax
import jax.numpy as jnp
import numpy as np
from jax import lax
from jax.experimental import pallas as pl
from jax.experimental.pallas import tpu as pltpu
from jax.sharding import Mesh
from jax.sharding import PartitionSpec as P

F32 = jnp.float32
BF16 = jnp.bfloat16
I32 = jnp.int32
AXES = ("gx", "gy_0", "gy_1", "gy_2")
GROUP = ("gy_1", "gy_2")
REST = ("gx", "gy_0")
OFFSETS = (1, 2, 3, 4, -1, -2, -3, -4)
MEMBERS = 16
PARTS = 3
OWN_ROWS = 64
LOCAL_ROWS = 96
FULL_ROWS = 98
GHOST_ROWS = 48


def lagrange(node_list, points):
    node_count = len(node_list)
    values = np.ones((len(points), node_count))
    derivs = np.zeros((len(points), node_count))
    for basis_node in range(node_count):
        for other_node in range(node_count):
            if other_node != basis_node:
                values[:, basis_node] = (
                    values[:, basis_node]
                    * (points - node_list[other_node])
                    / (node_list[basis_node] - node_list[other_node])
                )
        for skipped in range(node_count):
            if skipped != basis_node:
                product_term = np.ones(len(points)) / (node_list[basis_node] - node_list[skipped])
                for other_node in range(node_count):
                    if other_node != basis_node and other_node != skipped:
                        product_term = (
                            product_term
                            * (points - node_list[other_node])
                            / (node_list[basis_node] - node_list[other_node])
                        )
                derivs[:, basis_node] = derivs[:, basis_node] + product_term
    return (values, derivs)


def tables():
    gll_offset = np.sqrt(3.0 / 7.0)
    lobatto = np.array([0.0, (1.0 - gll_offset) / 2.0, 0.5, (1.0 + gll_offset) / 2.0, 1.0])
    inner_point = np.sqrt(5.0 - 2.0 * np.sqrt(10.0 / 7.0)) / 3.0
    outer_point = np.sqrt(5.0 + 2.0 * np.sqrt(10.0 / 7.0)) / 3.0
    inner_weight = (322.0 + 13.0 * np.sqrt(70.0)) / 900.0
    outer_weight = (322.0 - 13.0 * np.sqrt(70.0)) / 900.0
    points = np.array([-outer_point, -inner_point, 0.0, inner_point, outer_point])
    gauss_weights = np.array(
        [outer_weight, inner_weight, 128.0 / 225.0, inner_weight, outer_weight]
    )
    points = (points + 1.0) / 2.0
    gauss_weights = gauss_weights / 2.0
    shapes, slopes = lagrange(lobatto, points)
    fine_points = np.concatenate([lobatto / 2.0, (1.0 + lobatto) / 2.0])
    interp, _ = lagrange(lobatto, fine_points)
    quad_weights = np.kron(gauss_weights, np.kron(gauss_weights, gauss_weights))
    grad_x = np.kron(slopes, np.kron(shapes, shapes))
    grad_y = np.kron(shapes, np.kron(slopes, shapes))
    grad_z = np.kron(shapes, np.kron(shapes, slopes))
    stiffness = np.zeros((128, 128))
    for gradient in (grad_x, grad_y, grad_z):
        stiffness[:125, :125] += gradient.T @ (quad_weights[:, None] * gradient)
    interp_wide = np.zeros((8, 128))
    interp_wide[:5, :10] = interp.T
    return (jnp.asarray(interp_wide, F32), jnp.asarray(stiffness, F32))


def lane_pick(rows, lanes):
    return jnp.take_along_axis(rows, lanes, axis=1, mode="promise_in_bounds")


def pick(table, slots, first, last, picked=None):
    row_of = lax.shift_right_logical(slots, 7)
    lane_of = lax.bitwise_and(slots, 127)
    if picked is None:
        picked = jnp.zeros(slots.shape, F32)
    for row in range(first, last):
        spread_row = jnp.broadcast_to(table[row : row + 1, :], slots.shape)
        picked = jnp.where(row_of == row, lane_pick(spread_row, lane_of), picked)
    return picked


def split(x):
    pieces = []
    for part in range(PARTS):
        piece = x.astype(BF16)
        pieces.append(piece)
        if part + 1 < PARTS:
            x = x - piece.astype(F32)
    return pieces


def scatter(entries, first, rows):
    row_ids = lax.broadcasted_iota(I32, (rows, 128), 0).astype(F32).astype(BF16)
    lane_ids = lax.broadcasted_iota(I32, (128, 128), 0).astype(F32).astype(BF16)
    none = jnp.zeros((rows, 128), BF16)
    total = None
    for start in range(0, len(entries), 16):
        row_values = []
        lane_hots = []
        for slots, values in entries[start : start + 16]:
            row_of = (lax.shift_right_logical(slots, 7) - first).astype(F32).astype(BF16)
            lane_of = lax.bitwise_and(slots, 127).astype(F32).astype(BF16)
            row_hot = row_ids == jnp.broadcast_to(row_of, (rows, 128))
            lane_hot = lane_ids == jnp.broadcast_to(lane_of, (128, 128))
            row_values.append(
                jnp.concatenate(
                    [
                        jnp.where(row_hot, jnp.broadcast_to(piece, (rows, 128)), none)
                        for piece in split(values)
                    ],
                    axis=0,
                )
            )
            lane_hots.append(
                jnp.where(lane_hot, jnp.ones((128, 128), BF16), jnp.zeros((128, 128), BF16))
            )
        part = lax.dot_general(
            jnp.concatenate(row_values, axis=1),
            jnp.concatenate(lane_hots, axis=1),
            (((1,), (1,)), ((), ())),
            preferred_element_type=F32,
        )
        total = part if total is None else total + part
    result = total[:rows, :]
    for part in range(1, PARTS):
        result = result + total[rows * part : rows * part + rows, :]
    return result


def place_sends(place, sign, sends, pull):
    for member in range(MEMBERS):
        sends[member] = jnp.zeros(sends.shape[1:], F32)
    for block, offset in enumerate(OFFSETS):
        position = place + sign * offset
        outside = (position < 0) | (position >= MEMBERS)
        member = lax.bitwise_xor(
            lax.bitwise_and(position, MEMBERS - 1), jnp.where(outside, 1, 0)
        )
        for quarter, row in enumerate(pull(block)):
            sends[member, quarter : quarter + 1, :] = row


def arrived(place, received, relayed, offset, quarter):
    position = place + offset
    member = lax.bitwise_and(position, MEMBERS - 1)
    outside = (position < 0) | (position >= MEMBERS)
    inner = received[member, quarter : quarter + 1, :]
    outer = relayed[lax.bitwise_and(member, 3), quarter : quarter + 1, :]
    return jnp.where(outside, outer, inner)


def pick_lists(place, vector, lists, sends):
    quarters = [
        pick(vector, lists[:, 128 * quarter : 128 * quarter + 128], 0, OWN_ROWS)
        for quarter in range(4)
    ]
    place_sends(
        place, 1, sends, lambda block: [quarter[block : block + 1, :] for quarter in quarters]
    )


def first_kernel(place_ref, vector, lists, sends):
    pick_lists(place_ref[0], vector, lists, sends)


def near_kernel(vector, slots_in, masters_in, cell_part, master_part, slots, masters):
    slots[120:128, :] = jnp.zeros((8, 128), I32)
    slots[0:125, :] = slots_in[...]
    masters[...] = jnp.zeros((8, 256), I32)
    masters[0:5, :] = masters_in[...]
    for half in range(2):
        lanes = slice(128 * half, 128 * half + 128)
        master_part[:, lanes] = pick(vector, masters[:, lanes], 0, OWN_ROWS)
    for group in range(16):
        group_rows = slice(8 * group, 8 * group + 8)
        cell_part[group_rows, :] = pick(vector, slots[group_rows, :], 0, OWN_ROWS)


def con_weights(con_row, interp):
    return [
        lane_pick(
            interp[...],
            jnp.broadcast_to(con_row[:, 128 * half : 128 * half + 128], (8, 128)),
        )
        for half in range(2)
    ]


def cell_products(
    place,
    received,
    relayed,
    cell_part,
    master_part,
    slots,
    level,
    masters,
    con_row,
    interp,
    stiffness,
    table,
    cell_values,
    products,
):
    for block, offset in enumerate(OFFSETS):
        for quarter in range(4):
            row = OWN_ROWS + 4 * block + quarter
            table[row : row + 1, :] = arrived(place, received, relayed, -offset, quarter)
    for half, weight in enumerate(con_weights(con_row, interp)):
        lanes = slice(128 * half, 128 * half + 128)
        resolved = weight * pick(
            table, masters[:, lanes], OWN_ROWS, LOCAL_ROWS, master_part[:, lanes]
        )
        table[LOCAL_ROWS + half : LOCAL_ROWS + half + 1, :] = jnp.sum(
            resolved, axis=0, keepdims=True
        )
    for group in range(16):
        group_rows = slice(8 * group, 8 * group + 8)
        cell_values[group_rows, :] = pick(
            table, slots[group_rows, :], OWN_ROWS, FULL_ROWS, cell_part[group_rows, :]
        )
    products[...] = jnp.dot(
        stiffness[...],
        cell_values[...],
        precision=lax.Precision.HIGHEST,
        preferred_element_type=F32,
    ) * jnp.exp2(-level[...].astype(F32))


def cell_entries(slots, products):
    return [(slots[row : row + 1, :], products[row : row + 1, :]) for row in range(125)]


def con_entries(masters, back):
    return [
        (
            masters[node : node + 1, 128 * half : 128 * half + 128],
            back[node : node + 1, 128 * half : 128 * half + 128],
        )
        for node in range(5)
        for half in range(2)
    ]


def ghost_sums(place, slots, masters, con_row, interp, products, sends, back):
    spread = scatter(cell_entries(slots, products), OWN_ROWS, GHOST_ROWS)
    con_first = LOCAL_ROWS - OWN_ROWS
    for half, weight in enumerate(con_weights(con_row, interp)):
        sums = spread[con_first + half : con_first + half + 1, :]
        back[:, 128 * half : 128 * half + 128] = weight * jnp.broadcast_to(sums, (8, 128))
    spread = spread + scatter(con_entries(masters, back), OWN_ROWS, GHOST_ROWS)
    place_sends(
        place,
        -1,
        sends,
        lambda block: [spread[row : row + 1, :] for row in range(4 * block, 4 * block + 4)],
    )


def local_kernel(
    place_ref,
    received,
    relayed,
    cell_part,
    master_part,
    slots,
    level,
    masters,
    con_row,
    interp,
    stiffness,
    products,
    sends,
    back,
    table,
    cell_values,
):
    place = place_ref[0]
    cell_products(
        place,
        received,
        relayed,
        cell_part,
        master_part,
        slots,
        level,
        masters,
        con_row,
        interp,
        stiffness,
        table,
        cell_values,
        products,
    )
    ghost_sums(place, slots, masters, con_row, interp, products, sends, back)


def last_local_kernel(
    place_ref,
    received,
    relayed,
    cell_part,
    master_part,
    slots,
    level,
    masters,
    con_row,
    interp,
    stiffness,
    reaction,
    first,
    second,
    third,
    products,
    sends,
    back,
    table,
    cell_values,
):
    local_kernel(
        place_ref,
        received,
        relayed,
        cell_part,
        master_part,
        slots,
        level,
        masters,
        con_row,
        interp,
        stiffness,
        products,
        sends,
        back,
        table,
        cell_values,
    )
    vectors = [ref[...] for ref in (first, second, third)]
    sums = [jnp.sum(vectors[degree // 2] * vectors[(degree + 1) // 2]) for degree in range(5)]
    sums.append(
        jnp.sum(products[...] * cell_values[...])
        + jnp.sum(reaction[...] * vectors[2] * vectors[2])
    )
    lane = lax.broadcasted_iota(I32, (1, 128), 1)
    packed = jnp.zeros((1, 128), F32)
    for degree, value in enumerate(sums):
        packed = jnp.where(lane == degree, value, packed)
    for member in range(MEMBERS):
        sends[member, 4:5, :] = packed


def own_kernel(slots, masters, products, back, reaction, vector, own):
    spread = scatter(cell_entries(slots, products) + con_entries(masters, back), 0, OWN_ROWS)
    own[...] = spread + reaction[...] * vector[...]


def owner_sum(place, own, received, relayed, lists, vector):
    entries = [
        (
            lists[block : block + 1, 128 * quarter : 128 * quarter + 128],
            arrived(place, received, relayed, offset, quarter),
        )
        for block, offset in enumerate(OFFSETS)
        for quarter in range(4)
    ]
    vector[...] = own[...] + scatter(entries, 0, OWN_ROWS)


def owner_kernel(place_ref, own, received, relayed, lists, vector, sends):
    place = place_ref[0]
    owner_sum(place, own, received, relayed, lists, vector)
    pick_lists(place, vector, lists, sends)


def final_owner_kernel(place_ref, own, received, relayed, lists, vector):
    owner_sum(place_ref[0], own, received, relayed, lists, vector)


def last_kernel(moments, first, second, third, fourth, solution, residual):
    v = [ref[...] for ref in (first, second, third, fourth)]
    sums = moments[0]
    for member in range(1, moments.shape[0]):
        sums = sums + moments[member]
    lane = lax.broadcasted_iota(I32, (1, 128), 1)
    mu = [
        jnp.sum(jnp.where(lane == degree, sums, 0.0), axis=1, keepdims=True)
        for degree in range(6)
    ]
    zero = jnp.zeros((1, 1), F32)
    one = jnp.ones((1, 1), F32)

    def form(p, q, shift):
        value = zero
        for i, left in enumerate(p):
            for k, right in enumerate(q):
                value = value + left * right * mu[i + k + shift]
        return value

    res = [one]
    direction = [one]
    sol = [zero]
    rr = mu[0]
    for iteration in range(3):
        step = rr / form(direction, direction, 1)
        applied = [zero] + direction
        sol = [
            (sol[i] if i < len(sol) else zero) + step * direction[i]
            for i in range(len(direction))
        ]
        res = [
            (res[i] if i < len(res) else zero) - step * applied[i] for i in range(len(applied))
        ]
        if iteration < 2:
            rr_next = form(res, res, 0)
            ratio = rr_next / rr
            direction = [
                res[i] + (ratio * direction[i] if i < len(direction) else zero)
                for i in range(len(res))
            ]
            rr = rr_next
    solution[...] = sol[0] * v[0] + sol[1] * v[1] + sol[2] * v[2]
    residual[...] = res[0] * v[0] + res[1] * v[1] + res[2] * v[2] + res[3] * v[3]


def relay_pairs():
    pairs = []
    for group in range(32):
        for member in range(4):
            if group + 1 < 32:
                source = MEMBERS * group + member
                pairs.append((source, (source + MEMBERS) ^ 1))
            if group > 0:
                source = MEMBERS * group + 12 + member
                pairs.append((source, (source - MEMBERS) ^ 1))
    return pairs


def on_device(right_side, reaction, cell_slots, cell_level, con_masters, con_rows, send_lists):
    interp, stiffness = tables()
    place = lax.axis_index(GROUP).astype(I32)
    place_ref = place.reshape(1)
    whole = pl.BlockSpec(memory_space=pltpu.VMEM)
    scalar = pl.BlockSpec(memory_space=pltpu.SMEM)
    tile = jax.ShapeDtypeStruct((OWN_ROWS, 128), F32)
    sends = jax.ShapeDtypeStruct((MEMBERS, 4, 128), F32)
    vector = right_side.reshape(OWN_ROWS, 128)
    reaction = reaction.reshape(OWN_ROWS, 128)
    level = cell_level.reshape(1, 128)
    con_row = con_rows.reshape(1, 256)
    pairs = relay_pairs()

    def relay(received):
        first = jnp.where(place < 4, 12, 0)
        rows = lax.dynamic_slice(received, (first, 0, 0), (4, 4, 128))
        return lax.ppermute(rows, AXES, pairs)

    def kernel(body, outs, operands, scratch=(), outs_in_vmem=True):
        in_vmem = [
            operand
            if operand is place_ref
            else pltpu.with_memory_space_constraint(operand, pltpu.VMEM)
            for operand in operands
        ]
        return pl.pallas_call(
            body,
            out_shape=jax.tree.map(lambda out: pltpu.VMEM(out.shape, out.dtype), outs)
            if outs_in_vmem
            else outs,
            in_specs=[scalar if operand is place_ref else whole for operand in operands],
            out_specs=jax.tree.map(lambda out: whole, outs),
            scratch_shapes=scratch,
        )(*in_vmem)

    padded = jax.ShapeDtypeStruct((128, 128), F32)
    con_padded = jax.ShapeDtypeStruct((8, 256), F32)
    work = [pltpu.VMEM((104, 128), F32), pltpu.VMEM((128, 128), F32)]
    packed = kernel(first_kernel, sends, (place_ref, vector, send_lists))
    vectors = [vector]
    for step in range(3):
        vector = vectors[-1]
        received = lax.all_to_all(packed, GROUP, 0, 0)
        cell_part, master_part, slots, masters = kernel(
            near_kernel,
            (
                padded,
                con_padded,
                jax.ShapeDtypeStruct((128, 128), I32),
                jax.ShapeDtypeStruct((8, 256), I32),
            ),
            (vector, cell_slots, con_masters),
        )
        relayed = relay(received)
        operands = (
            place_ref,
            received,
            relayed,
            cell_part,
            master_part,
            slots,
            level,
            masters,
            con_row,
            interp,
            stiffness,
        )
        if step < 2:
            products, packed, back = kernel(
                local_kernel, (padded, sends, con_padded), operands, work
            )
        else:
            products, packed, back = kernel(
                last_local_kernel,
                (padded, jax.ShapeDtypeStruct((MEMBERS, 8, 128), F32), con_padded),
                operands + (reaction,) + tuple(vectors),
                work,
            )
        received = lax.all_to_all(packed, GROUP, 0, 0)
        own = kernel(own_kernel, tile, (slots, masters, products, back, reaction, vector))
        relayed = relay(received)
        if step < 2:
            vector, packed = kernel(
                owner_kernel, (tile, sends), (place_ref, own, received, relayed, send_lists)
            )
            vectors.append(vector)
        else:
            sums = jnp.broadcast_to(jnp.sum(received[:, 4:5, :], axis=0)[None], (32, 1, 128))
            moments = lax.all_to_all(sums, REST, 0, 0)
            vector = kernel(
                final_owner_kernel, tile, (place_ref, own, received, relayed, send_lists)
            )
            vectors.append(vector)
    solution_rows, residual_rows = kernel(
        last_kernel, (tile, tile), (moments, *vectors), outs_in_vmem=False
    )
    return (solution_rows.reshape(-1), residual_rows.reshape(-1))


def solution(mesh):
    torus = Mesh(mesh.devices.reshape(mesh.shape["gx"], 4, 8, 2), AXES)
    placed = (
        P(AXES),
        P(AXES),
        P(None, AXES),
        P(AXES),
        P(None, AXES),
        P(AXES),
        P(None, AXES),
    )
    return jax.shard_map(
        on_device, mesh=torus, in_specs=placed, out_specs=(P(AXES), P(AXES)), check_vma=False
    )
```

```python
import jax
import jax.numpy as jnp
import numpy as np
from jax import lax
from jax.experimental import pallas as pl
from jax.experimental.pallas import tpu as pltpu
from jax.sharding import Mesh
from jax.sharding import PartitionSpec as P

F32 = jnp.float32
BF16 = jnp.bfloat16
I32 = jnp.int32
AXES = ("gx", "gy_0", "gy_1", "gy_2")
GROUP = ("gy_1", "gy_2")
REST = ("gx", "gy_0")
OFFSETS = (1, 2, 3, 4, -1, -2, -3, -4)
MEMBERS = 16
PARTS = 3
OWN_ROWS = 64
LOCAL_ROWS = 96
GHOST_ROWS = 34


def lagrange(node_list, points):
    node_count = len(node_list)
    values = np.ones((len(points), node_count))
    derivs = np.zeros((len(points), node_count))
    for basis_node in range(node_count):
        for other_node in range(node_count):
            if other_node != basis_node:
                values[:, basis_node] = (
                    values[:, basis_node]
                    * (points - node_list[other_node])
                    / (node_list[basis_node] - node_list[other_node])
                )
        for skipped in range(node_count):
            if skipped != basis_node:
                product_term = np.ones(len(points)) / (node_list[basis_node] - node_list[skipped])
                for other_node in range(node_count):
                    if other_node != basis_node and other_node != skipped:
                        product_term = (
                            product_term
                            * (points - node_list[other_node])
                            / (node_list[basis_node] - node_list[other_node])
                        )
                derivs[:, basis_node] = derivs[:, basis_node] + product_term
    return (values, derivs)


def tables():
    gll_offset = np.sqrt(3.0 / 7.0)
    lobatto = np.array([0.0, (1.0 - gll_offset) / 2.0, 0.5, (1.0 + gll_offset) / 2.0, 1.0])
    inner_point = np.sqrt(5.0 - 2.0 * np.sqrt(10.0 / 7.0)) / 3.0
    outer_point = np.sqrt(5.0 + 2.0 * np.sqrt(10.0 / 7.0)) / 3.0
    inner_weight = (322.0 + 13.0 * np.sqrt(70.0)) / 900.0
    outer_weight = (322.0 - 13.0 * np.sqrt(70.0)) / 900.0
    points = np.array([-outer_point, -inner_point, 0.0, inner_point, outer_point])
    gauss_weights = np.array(
        [outer_weight, inner_weight, 128.0 / 225.0, inner_weight, outer_weight]
    )
    points = (points + 1.0) / 2.0
    gauss_weights = gauss_weights / 2.0
    shapes, slopes = lagrange(lobatto, points)
    fine_points = np.concatenate([lobatto / 2.0, (1.0 + lobatto) / 2.0])
    interp, _ = lagrange(lobatto, fine_points)
    quad_weights = np.kron(gauss_weights, np.kron(gauss_weights, gauss_weights))
    grad_x = np.kron(slopes, np.kron(shapes, shapes))
    grad_y = np.kron(shapes, np.kron(slopes, shapes))
    grad_z = np.kron(shapes, np.kron(shapes, slopes))
    stiffness = np.zeros((128, 128))
    for gradient in (grad_x, grad_y, grad_z):
        stiffness[:125, :125] += gradient.T @ (quad_weights[:, None] * gradient)
    interp_wide = np.zeros((8, 128))
    interp_wide[:5, :10] = interp.T
    return (jnp.asarray(interp_wide, F32), jnp.asarray(stiffness, F32))


def lane_pick(rows, lanes):
    return jnp.take_along_axis(rows, lanes, axis=1, mode="promise_in_bounds")


def pick(table, slots, first, last, picked=None, base=0):
    row_of = lax.shift_right_logical(slots, 7)
    lane_of = lax.bitwise_and(slots, 127)
    if picked is None:
        picked = jnp.zeros(slots.shape, F32)
    for row in range(first, last):
        spread_row = jnp.broadcast_to(table[row : row + 1, :], slots.shape)
        picked = jnp.where(row_of == base + row, lane_pick(spread_row, lane_of), picked)
    return picked


def split(x):
    pieces = []
    for part in range(PARTS):
        piece = x.astype(BF16)
        pieces.append(piece)
        if part + 1 < PARTS:
            x = x - piece.astype(F32)
    return pieces


def stacked(pieces, rows, tall):
    blocks = []
    for base in range(0, tall, 16):
        low = min(base // rows, PARTS - 1)
        high = min((base + 15) // rows, PARTS - 1)
        block = jnp.broadcast_to(pieces[low], (16, 128))
        if high > low:
            ids = lax.broadcasted_iota(I32, (16, 128), 0).astype(F32).astype(BF16)
            block = jnp.where(
                ids < jnp.full((16, 128), high * rows - base, BF16),
                block,
                jnp.broadcast_to(pieces[high], (16, 128)),
            )
        blocks.append(block)
    return jnp.concatenate(blocks, axis=0)


def scatter(entries, first, rows):
    tall = -(-PARTS * rows // 16) * 16
    row_ids = lax.broadcasted_iota(I32, (tall, 128), 0)
    row_ids = jnp.where(
        row_ids >= PARTS * rows,
        -256,
        row_ids - jnp.where(row_ids >= 2 * rows, 2 * rows, jnp.where(row_ids >= rows, rows, 0)),
    )
    row_ids = row_ids.astype(F32).astype(BF16)
    lane_ids = lax.broadcasted_iota(I32, (128, 128), 0).astype(F32).astype(BF16)
    none = jnp.zeros((tall, 128), BF16)
    total = None
    for start in range(0, len(entries), 16):
        row_values = []
        lane_hots = []
        for slots, values in entries[start : start + 16]:
            row_of = (lax.shift_right_logical(slots, 7) - first).astype(F32).astype(BF16)
            lane_of = lax.bitwise_and(slots, 127).astype(F32).astype(BF16)
            row_hot = row_ids == jnp.broadcast_to(row_of, (tall, 128))
            lane_hot = lane_ids == jnp.broadcast_to(lane_of, (128, 128))
            row_values.append(jnp.where(row_hot, stacked(split(values), rows, tall), none))
            lane_hots.append(
                jnp.where(lane_hot, jnp.ones((128, 128), BF16), jnp.zeros((128, 128), BF16))
            )
        part = lax.dot_general(
            jnp.concatenate(row_values, axis=1),
            jnp.concatenate(lane_hots, axis=1),
            (((1,), (1,)), ((), ())),
            preferred_element_type=F32,
        )
        total = part if total is None else total + part
    result = total[:rows, :]
    for part in range(1, PARTS):
        result = result + total[rows * part : rows * part + rows, :]
    return result


def place_sends(place, sign, sends, pull):
    for member in range(MEMBERS):
        sends[member] = jnp.zeros(sends.shape[1:], F32)
    for block, offset in enumerate(OFFSETS):
        position = place + sign * offset
        outside = (position < 0) | (position >= MEMBERS)
        member = lax.bitwise_xor(
            lax.bitwise_and(position, MEMBERS - 1), jnp.where(outside, 1, 0)
        )
        for quarter, row in enumerate(pull(block)):
            sends[member, quarter : quarter + 1, :] = row


def arrived(place, received, relayed, offset, quarter):
    position = place + offset
    member = lax.bitwise_and(position, MEMBERS - 1)
    outside = (position < 0) | (position >= MEMBERS)
    inner = received[member, quarter : quarter + 1, :]
    outer = relayed[lax.bitwise_and(member, 3), quarter : quarter + 1, :]
    return jnp.where(outside, outer, inner)


def pick_lists(place, vector, lists, sends):
    quarters = [
        pick(vector, lists[:, 128 * quarter : 128 * quarter + 128], 0, OWN_ROWS)
        for quarter in range(4)
    ]
    place_sends(
        place, 1, sends, lambda block: [quarter[block : block + 1, :] for quarter in quarters]
    )


def first_kernel(
    place_ref,
    vector_in,
    lists,
    slots_in,
    masters_in,
    con_row,
    level,
    interp,
    stiffness_in,
    reaction_in,
    sends,
    vector,
    slots,
    masters,
    weights,
    scale,
    stiffness,
    reaction,
):
    vector[...] = vector_in[...]
    pick_lists(place_ref[0], vector_in, lists, sends)
    slots[120:128, :] = jnp.zeros((8, 128), I32)
    slots[0:125, :] = slots_in[...]
    masters[...] = jnp.zeros((8, 256), I32)
    masters[0:5, :] = masters_in[...]
    for half in range(2):
        lanes = slice(128 * half, 128 * half + 128)
        weights[:, lanes] = lane_pick(
            interp[...], jnp.broadcast_to(con_row[:, lanes], (8, 128))
        )
    scale[...] = jnp.exp2(-level[...].astype(F32))
    stiffness[...] = stiffness_in[...]
    reaction[...] = reaction_in[...]


def near_kernel(place_ref, vector, received, slots, masters, cell_part, master_part, table):
    place = place_ref[0]
    table[0:OWN_ROWS, :] = vector[...]
    for block, offset in enumerate(OFFSETS):
        member = lax.bitwise_and(place - offset, MEMBERS - 1)
        for quarter in range(4):
            row = OWN_ROWS + 4 * block + quarter
            table[row : row + 1, :] = received[member, quarter : quarter + 1, :]
    for half in range(2):
        lanes = slice(128 * half, 128 * half + 128)
        master_part[:, lanes] = pick(table, masters[:, lanes], 0, LOCAL_ROWS)
    for group in range(16):
        group_rows = slice(8 * group, 8 * group + 8)
        cell_part[group_rows, :] = pick(table, slots[group_rows, :], 0, LOCAL_ROWS)


def cell_products(
    place,
    received,
    relayed,
    cell_part,
    master_part,
    slots,
    scale,
    masters,
    weights,
    stiffness,
    table,
    cell_values,
    products,
):
    forward = place < 8
    base = jnp.where(forward, OWN_ROWS, OWN_ROWS + 16)
    for block in range(4):
        offset = jnp.where(forward, block + 1, -(block + 1))
        for quarter in range(4):
            row = 4 * block + quarter
            table[row : row + 1, :] = arrived(place, received, relayed, -offset, quarter)
    for half in range(2):
        lanes = slice(128 * half, 128 * half + 128)
        resolved = weights[:, lanes] * pick(
            table, masters[:, lanes], 0, 16, master_part[:, lanes], base
        )
        table[16 + half : 17 + half, :] = jnp.sum(resolved, axis=0, keepdims=True)
    for group in range(16):
        group_rows = slice(8 * group, 8 * group + 8)
        at = slots[group_rows, :]
        values = pick(table, at, 0, 16, cell_part[group_rows, :], base)
        cell_values[group_rows, :] = pick(table, at, 16, 18, values, LOCAL_ROWS - 16)
    products[...] = jnp.dot(
        stiffness[...],
        cell_values[...],
        precision=lax.Precision.HIGHEST,
        preferred_element_type=F32,
    ) * scale[...]


def cell_entries(slots, products):
    return [(slots[row : row + 1, :], products[row : row + 1, :]) for row in range(125)]


def con_entries(masters, back):
    return [
        (
            masters[node : node + 1, 128 * half : 128 * half + 128],
            back[node : node + 1, 128 * half : 128 * half + 128],
        )
        for node in range(5)
        for half in range(2)
    ]


def ghost_sums(place, slots, masters, weights, products, sends, back):
    spread = scatter(cell_entries(slots, products), OWN_ROWS, GHOST_ROWS)
    con_first = LOCAL_ROWS - OWN_ROWS
    for half in range(2):
        lanes = slice(128 * half, 128 * half + 128)
        sums = spread[con_first + half : con_first + half + 1, :]
        back[:, lanes] = weights[:, lanes] * jnp.broadcast_to(sums, (8, 128))
    spread = spread + scatter(con_entries(masters, back), OWN_ROWS, GHOST_ROWS)
    place_sends(
        place,
        -1,
        sends,
        lambda block: [spread[row : row + 1, :] for row in range(4 * block, 4 * block + 4)],
    )


def local_kernel(
    place_ref,
    received,
    relayed,
    cell_part,
    master_part,
    slots,
    scale,
    masters,
    weights,
    stiffness,
    products,
    sends,
    back,
    table,
    cell_values,
):
    place = place_ref[0]
    cell_products(
        place,
        received,
        relayed,
        cell_part,
        master_part,
        slots,
        scale,
        masters,
        weights,
        stiffness,
        table,
        cell_values,
        products,
    )
    ghost_sums(place, slots, masters, weights, products, sends, back)


def last_local_kernel(
    place_ref,
    received,
    relayed,
    cell_part,
    master_part,
    slots,
    scale,
    masters,
    weights,
    stiffness,
    reaction,
    first,
    second,
    third,
    products,
    sends,
    back,
    table,
    cell_values,
):
    local_kernel(
        place_ref,
        received,
        relayed,
        cell_part,
        master_part,
        slots,
        scale,
        masters,
        weights,
        stiffness,
        products,
        sends,
        back,
        table,
        cell_values,
    )
    vectors = [ref[...] for ref in (first, second, third)]
    sums = [jnp.sum(vectors[degree // 2] * vectors[(degree + 1) // 2]) for degree in range(5)]
    sums.append(
        jnp.sum(products[...] * cell_values[...])
        + jnp.sum(reaction[...] * vectors[2] * vectors[2])
    )
    lane = lax.broadcasted_iota(I32, (1, 128), 1)
    packed = jnp.zeros((1, 128), F32)
    for degree, value in enumerate(sums):
        packed = jnp.where(lane == degree, value, packed)
    for member in range(MEMBERS):
        sends[member, 4:5, :] = packed


def own_kernel(
    place_ref, slots, masters, products, back, reaction, vector, received, lists, own
):
    place = place_ref[0]
    entries = cell_entries(slots, products) + con_entries(masters, back)
    for block, offset in enumerate(OFFSETS):
        position = place + offset
        inside = (position >= 0) & (position < MEMBERS)
        member = lax.bitwise_and(position, MEMBERS - 1)
        for quarter in range(4):
            row = received[member, quarter : quarter + 1, :]
            entries.append(
                (
                    lists[block : block + 1, 128 * quarter : 128 * quarter + 128],
                    jnp.where(inside, row, 0.0),
                )
            )
    own[...] = scatter(entries, 0, OWN_ROWS) + reaction[...] * vector[...]


def owner_sum(place, own, relayed, lists, vector):
    entries = []
    back = place < 8
    for block in range(4):
        position = jnp.where(back, place - (block + 1), place + block + 1)
        outside = (position < 0) | (position >= MEMBERS)
        member = lax.bitwise_and(position, 3)
        for quarter in range(4):
            lanes = slice(128 * quarter, 128 * quarter + 128)
            slots = jnp.where(
                back, lists[block + 4 : block + 5, lanes], lists[block : block + 1, lanes]
            )
            row = relayed[member, quarter : quarter + 1, :]
            entries.append((slots, jnp.where(outside, row, 0.0)))
    vector[...] = own[...] + scatter(entries, 0, OWN_ROWS)


def owner_kernel(place_ref, own, relayed, lists, vector, sends):
    place = place_ref[0]
    owner_sum(place, own, relayed, lists, vector)
    pick_lists(place, vector, lists, sends)


def final_owner_kernel(place_ref, own, relayed, lists, vector):
    owner_sum(place_ref[0], own, relayed, lists, vector)


def group_kernel(received, sums):
    total = received[0, 4:5, :]
    for member in range(1, MEMBERS):
        total = total + received[member, 4:5, :]
    for member in range(sums.shape[0]):
        sums[member] = total


def last_kernel(moments, first, second, third, fourth, solution, residual):
    v = [ref[...] for ref in (first, second, third, fourth)]
    sums = moments[0]
    for member in range(1, moments.shape[0]):
        sums = sums + moments[member]
    lane = lax.broadcasted_iota(I32, (1, 128), 1)
    mu = [
        jnp.sum(jnp.where(lane == degree, sums, 0.0), axis=1, keepdims=True)
        for degree in range(6)
    ]
    zero = jnp.zeros((1, 1), F32)
    one = jnp.ones((1, 1), F32)

    def form(p, q, shift):
        value = zero
        for i, left in enumerate(p):
            for k, right in enumerate(q):
                value = value + left * right * mu[i + k + shift]
        return value

    res = [one]
    direction = [one]
    sol = [zero]
    rr = mu[0]
    for iteration in range(3):
        step = rr / form(direction, direction, 1)
        applied = [zero] + direction
        sol = [
            (sol[i] if i < len(sol) else zero) + step * direction[i]
            for i in range(len(direction))
        ]
        res = [
            (res[i] if i < len(res) else zero) - step * applied[i] for i in range(len(applied))
        ]
        if iteration < 2:
            rr_next = form(res, res, 0)
            ratio = rr_next / rr
            direction = [
                res[i] + (ratio * direction[i] if i < len(direction) else zero)
                for i in range(len(res))
            ]
            rr = rr_next
    solution[...] = sol[0] * v[0] + sol[1] * v[1] + sol[2] * v[2]
    residual[...] = res[0] * v[0] + res[1] * v[1] + res[2] * v[2] + res[3] * v[3]


def relay_pairs():
    pairs = []
    for group in range(32):
        for member in range(4):
            if group + 1 < 32:
                source = MEMBERS * group + member
                pairs.append((source, (source + MEMBERS) ^ 1))
            if group > 0:
                source = MEMBERS * group + 12 + member
                pairs.append((source, (source - MEMBERS) ^ 1))
    return pairs


def on_device(right_side, reaction, cell_slots, cell_level, con_masters, con_rows, send_lists):
    interp, stiffness = tables()
    place = lax.axis_index(GROUP).astype(I32)
    place_ref, relay_first = lax.optimization_barrier(
        (place.reshape(1), jnp.where(place < 4, 12, 0).astype(I32))
    )
    whole = pl.BlockSpec(memory_space=pltpu.VMEM)
    scalar = pl.BlockSpec(memory_space=pltpu.SMEM)
    tile = jax.ShapeDtypeStruct((OWN_ROWS, 128), F32)
    sends = jax.ShapeDtypeStruct((MEMBERS, 4, 128), F32)
    vector = right_side.reshape(OWN_ROWS, 128)
    reaction = reaction.reshape(OWN_ROWS, 128)
    level = cell_level.reshape(1, 128)
    con_row = con_rows.reshape(1, 256)
    pairs = relay_pairs()

    def relay(received):
        rows = lax.dynamic_slice(received, (relay_first, 0, 0), (4, 4, 128))
        return lax.ppermute(rows, AXES, pairs)

    def kernel(body, outs, operands, scratch=(), ins_in_vmem=True, outs_in_vmem=True):
        in_vmem = [
            operand
            if operand is place_ref or not ins_in_vmem
            else pltpu.with_memory_space_constraint(operand, pltpu.VMEM)
            for operand in operands
        ]
        return pl.pallas_call(
            body,
            out_shape=jax.tree.map(lambda out: pltpu.VMEM(out.shape, out.dtype), outs)
            if outs_in_vmem
            else outs,
            in_specs=[scalar if operand is place_ref else whole for operand in operands],
            out_specs=jax.tree.map(lambda out: whole, outs),
            scratch_shapes=scratch,
        )(*in_vmem)

    padded = jax.ShapeDtypeStruct((128, 128), F32)
    con_padded = jax.ShapeDtypeStruct((8, 256), F32)
    work = [pltpu.VMEM((24, 128), F32), pltpu.VMEM((128, 128), F32)]
    packed, vector, slots, masters, weights, scale, stiffness, reaction = kernel(
        first_kernel,
        (
            sends,
            tile,
            jax.ShapeDtypeStruct((128, 128), I32),
            jax.ShapeDtypeStruct((8, 256), I32),
            con_padded,
            jax.ShapeDtypeStruct((1, 128), F32),
            padded,
            tile,
        ),
        (
            place_ref,
            vector,
            send_lists,
            cell_slots,
            con_masters,
            con_row,
            level,
            interp,
            stiffness,
            reaction,
        ),
        ins_in_vmem=False,
    )
    vectors = [vector]
    for step in range(3):
        vector = vectors[-1]
        received = lax.all_to_all(packed, GROUP, 0, 0)
        cell_part, master_part = kernel(
            near_kernel,
            (padded, con_padded),
            (place_ref, vector, received, slots, masters),
            [pltpu.VMEM((LOCAL_ROWS, 128), F32)],
        )
        relayed = relay(received)
        operands = (
            place_ref,
            received,
            relayed,
            cell_part,
            master_part,
            slots,
            scale,
            masters,
            weights,
            stiffness,
        )
        if step < 2:
            products, packed, back = kernel(
                local_kernel, (padded, sends, con_padded), operands, work
            )
        else:
            products, packed, back = kernel(
                last_local_kernel,
                (padded, jax.ShapeDtypeStruct((MEMBERS, 8, 128), F32), con_padded),
                operands + (reaction,) + tuple(vectors),
                work,
            )
        received = lax.all_to_all(packed, GROUP, 0, 0)
        own = kernel(
            own_kernel,
            tile,
            (place_ref, slots, masters, products, back, reaction, vector, received, send_lists),
        )
        relayed = relay(received)
        if step < 2:
            vector, packed = kernel(
                owner_kernel, (tile, sends), (place_ref, own, relayed, send_lists)
            )
            vectors.append(vector)
        else:
            sums = kernel(group_kernel, jax.ShapeDtypeStruct((32, 1, 128), F32), (received,))
            moments = lax.all_to_all(sums, REST, 0, 0)
            vector = kernel(final_owner_kernel, tile, (place_ref, own, relayed, send_lists))
            vectors.append(vector)
    solution_rows, residual_rows = kernel(
        last_kernel, (tile, tile), (moments, *vectors), outs_in_vmem=False
    )
    return (solution_rows.reshape(-1), residual_rows.reshape(-1))


def solution(mesh):
    torus = Mesh(mesh.devices.reshape(mesh.shape["gx"], 4, 8, 2), AXES)
    placed = (
        P(AXES),
        P(AXES),
        P(None, AXES),
        P(AXES),
        P(None, AXES),
        P(AXES),
        P(None, AXES),
    )
    return jax.shard_map(
        on_device, mesh=torus, in_specs=placed, out_specs=(P(AXES), P(AXES)), check_vma=False
    )
```

```python
import jax
import jax.numpy as jnp
import numpy as np
from jax import lax
from jax.experimental import pallas as pl
from jax.experimental.pallas import tpu as pltpu
from jax.sharding import Mesh
from jax.sharding import PartitionSpec as P

F32 = jnp.float32
BF16 = jnp.bfloat16
I32 = jnp.int32
AXES = ("gx", "gy_0", "gy_1", "gy_2")
GROUP = ("gy_1", "gy_2")
REST = ("gx", "gy_0")
OFFSETS = (1, 2, 3, 4, -1, -2, -3, -4)
MEMBERS = 16
PARTS = 3
OWN_ROWS = 64
LOCAL_ROWS = 96
GHOST_ROWS = 34


def lagrange(node_list, points):
    node_count = len(node_list)
    values = np.ones((len(points), node_count))
    derivs = np.zeros((len(points), node_count))
    for basis_node in range(node_count):
        for other_node in range(node_count):
            if other_node != basis_node:
                values[:, basis_node] = (
                    values[:, basis_node]
                    * (points - node_list[other_node])
                    / (node_list[basis_node] - node_list[other_node])
                )
        for skipped in range(node_count):
            if skipped != basis_node:
                product_term = np.ones(len(points)) / (node_list[basis_node] - node_list[skipped])
                for other_node in range(node_count):
                    if other_node != basis_node and other_node != skipped:
                        product_term = (
                            product_term
                            * (points - node_list[other_node])
                            / (node_list[basis_node] - node_list[other_node])
                        )
                derivs[:, basis_node] = derivs[:, basis_node] + product_term
    return (values, derivs)


def tables():
    gll_offset = np.sqrt(3.0 / 7.0)
    lobatto = np.array([0.0, (1.0 - gll_offset) / 2.0, 0.5, (1.0 + gll_offset) / 2.0, 1.0])
    inner_point = np.sqrt(5.0 - 2.0 * np.sqrt(10.0 / 7.0)) / 3.0
    outer_point = np.sqrt(5.0 + 2.0 * np.sqrt(10.0 / 7.0)) / 3.0
    inner_weight = (322.0 + 13.0 * np.sqrt(70.0)) / 900.0
    outer_weight = (322.0 - 13.0 * np.sqrt(70.0)) / 900.0
    points = np.array([-outer_point, -inner_point, 0.0, inner_point, outer_point])
    gauss_weights = np.array(
        [outer_weight, inner_weight, 128.0 / 225.0, inner_weight, outer_weight]
    )
    points = (points + 1.0) / 2.0
    gauss_weights = gauss_weights / 2.0
    shapes, slopes = lagrange(lobatto, points)
    fine_points = np.concatenate([lobatto / 2.0, (1.0 + lobatto) / 2.0])
    interp, _ = lagrange(lobatto, fine_points)
    quad_weights = np.kron(gauss_weights, np.kron(gauss_weights, gauss_weights))
    grad_x = np.kron(slopes, np.kron(shapes, shapes))
    grad_y = np.kron(shapes, np.kron(slopes, shapes))
    grad_z = np.kron(shapes, np.kron(shapes, slopes))
    stiffness = np.zeros((128, 128))
    for gradient in (grad_x, grad_y, grad_z):
        stiffness[:125, :125] += gradient.T @ (quad_weights[:, None] * gradient)
    interp_wide = np.zeros((8, 128))
    interp_wide[:5, :10] = interp.T
    return (jnp.asarray(interp_wide, F32), jnp.asarray(stiffness, F32))


def lane_pick(rows, lanes):
    return jnp.take_along_axis(rows, lanes, axis=1, mode="promise_in_bounds")


def pick(table, slots, first, last, picked=None, base=0):
    row_of = lax.shift_right_logical(slots, 7)
    lane_of = lax.bitwise_and(slots, 127)
    if picked is None:
        picked = jnp.zeros(slots.shape, F32)
    for row in range(first, last):
        spread_row = jnp.broadcast_to(table[row : row + 1, :], slots.shape)
        picked = jnp.where(row_of == base + row, lane_pick(spread_row, lane_of), picked)
    return picked


def split(x):
    pieces = []
    for part in range(PARTS):
        piece = x.astype(BF16)
        pieces.append(piece)
        if part + 1 < PARTS:
            x = x - piece.astype(F32)
    return pieces


def stacked(pieces, rows, tall):
    blocks = []
    for base in range(0, tall, 16):
        low = min(base // rows, PARTS - 1)
        high = min((base + 15) // rows, PARTS - 1)
        block = jnp.broadcast_to(pieces[low], (16, 128))
        if high > low:
            ids = lax.broadcasted_iota(I32, (16, 128), 0).astype(F32).astype(BF16)
            block = jnp.where(
                ids < jnp.full((16, 128), high * rows - base, BF16),
                block,
                jnp.broadcast_to(pieces[high], (16, 128)),
            )
        blocks.append(block)
    return jnp.concatenate(blocks, axis=0)


def scatter(entries, first, rows):
    tall = -(-PARTS * rows // 16) * 16
    row_ids = lax.broadcasted_iota(I32, (tall, 128), 0)
    row_ids = jnp.where(
        row_ids >= PARTS * rows,
        -256,
        row_ids - jnp.where(row_ids >= 2 * rows, 2 * rows, jnp.where(row_ids >= rows, rows, 0)),
    )
    row_ids = row_ids.astype(F32).astype(BF16)
    lane_ids = lax.broadcasted_iota(I32, (128, 128), 0).astype(F32).astype(BF16)
    none = jnp.zeros((tall, 128), BF16)
    total = None
    for start in range(0, len(entries), 16):
        row_values = []
        lane_hots = []
        for slots, values in entries[start : start + 16]:
            row_of = (lax.shift_right_logical(slots, 7) - first).astype(F32).astype(BF16)
            lane_of = lax.bitwise_and(slots, 127).astype(F32).astype(BF16)
            row_hot = row_ids == jnp.broadcast_to(row_of, (tall, 128))
            lane_hot = lane_ids == jnp.broadcast_to(lane_of, (128, 128))
            row_values.append(jnp.where(row_hot, stacked(split(values), rows, tall), none))
            lane_hots.append(
                jnp.where(lane_hot, jnp.ones((128, 128), BF16), jnp.zeros((128, 128), BF16))
            )
        part = lax.dot_general(
            jnp.concatenate(row_values, axis=1),
            jnp.concatenate(lane_hots, axis=1),
            (((1,), (1,)), ((), ())),
            preferred_element_type=F32,
        )
        total = part if total is None else total + part
    result = total[:rows, :]
    for part in range(1, PARTS):
        result = result + total[rows * part : rows * part + rows, :]
    return result


def place_sends(place, sign, sends, pull):
    for member in range(MEMBERS):
        sends[member] = jnp.zeros(sends.shape[1:], F32)
    for block, offset in enumerate(OFFSETS):
        position = place + sign * offset
        outside = (position < 0) | (position >= MEMBERS)
        member = lax.bitwise_xor(
            lax.bitwise_and(position, MEMBERS - 1), jnp.where(outside, 1, 0)
        )
        for quarter, row in enumerate(pull(block)):
            sends[member, quarter : quarter + 1, :] = row


def arrived(place, received, relayed, offset, quarter):
    position = place + offset
    member = lax.bitwise_and(position, MEMBERS - 1)
    outside = (position < 0) | (position >= MEMBERS)
    inner = received[member, quarter : quarter + 1, :]
    outer = relayed[lax.bitwise_and(member, 3), quarter : quarter + 1, :]
    return jnp.where(outside, outer, inner)


def pick_lists(place, vector, lists, sends):
    quarters = [
        pick(vector, lists[:, 128 * quarter : 128 * quarter + 128], 0, OWN_ROWS)
        for quarter in range(4)
    ]
    place_sends(
        place, 1, sends, lambda block: [quarter[block : block + 1, :] for quarter in quarters]
    )


def first_kernel(
    place_ref,
    vector_in,
    lists,
    slots_in,
    masters_in,
    con_row,
    level,
    interp,
    stiffness_in,
    reaction_in,
    sends,
    vector,
    slots,
    masters,
    weights,
    scale,
    stiffness,
    reaction,
):
    vector[...] = vector_in[...]
    pick_lists(place_ref[0], vector_in, lists, sends)
    slots[120:128, :] = jnp.zeros((8, 128), I32)
    slots[0:125, :] = slots_in[...]
    masters[...] = jnp.zeros((8, 256), I32)
    masters[0:5, :] = masters_in[...]
    for half in range(2):
        lanes = slice(128 * half, 128 * half + 128)
        weights[:, lanes] = lane_pick(
            interp[...], jnp.broadcast_to(con_row[:, lanes], (8, 128))
        )
    scale[...] = jnp.exp2(-level[...].astype(F32))
    stiffness[...] = stiffness_in[...]
    reaction[...] = reaction_in[...]


def near_kernel(place_ref, vector, received, slots, masters, cell_part, master_part, table):
    place = place_ref[0]
    table[0:OWN_ROWS, :] = vector[...]
    for block, offset in enumerate(OFFSETS):
        member = lax.bitwise_and(place - offset, MEMBERS - 1)
        for quarter in range(4):
            row = OWN_ROWS + 4 * block + quarter
            table[row : row + 1, :] = received[member, quarter : quarter + 1, :]
    for half in range(2):
        lanes = slice(128 * half, 128 * half + 128)
        master_part[:, lanes] = pick(table, masters[:, lanes], 0, LOCAL_ROWS)
    for group in range(16):
        group_rows = slice(8 * group, 8 * group + 8)
        cell_part[group_rows, :] = pick(table, slots[group_rows, :], 0, LOCAL_ROWS)


def cell_products(
    place,
    received,
    relayed,
    cell_part,
    master_part,
    slots,
    scale,
    masters,
    weights,
    stiffness,
    table,
    cell_values,
    products,
):
    forward = place < 8
    base = jnp.where(forward, OWN_ROWS, OWN_ROWS + 16)
    for block in range(4):
        offset = jnp.where(forward, block + 1, -(block + 1))
        for quarter in range(4):
            row = 4 * block + quarter
            table[row : row + 1, :] = arrived(place, received, relayed, -offset, quarter)
    for half in range(2):
        lanes = slice(128 * half, 128 * half + 128)
        resolved = weights[:, lanes] * pick(
            table, masters[:, lanes], 0, 16, master_part[:, lanes], base
        )
        table[16 + half : 17 + half, :] = jnp.sum(resolved, axis=0, keepdims=True)
    for group in range(16):
        group_rows = slice(8 * group, 8 * group + 8)
        at = slots[group_rows, :]
        values = pick(table, at, 0, 16, cell_part[group_rows, :], base)
        cell_values[group_rows, :] = pick(table, at, 16, 18, values, LOCAL_ROWS - 16)
    products[...] = jnp.dot(
        stiffness[...],
        cell_values[...],
        precision=lax.Precision.HIGHEST,
        preferred_element_type=F32,
    ) * scale[...]


def cell_entries(slots, products):
    return [(slots[row : row + 1, :], products[row : row + 1, :]) for row in range(125)]


def con_entries(masters, back):
    return [
        (
            masters[node : node + 1, 128 * half : 128 * half + 128],
            back[node : node + 1, 128 * half : 128 * half + 128],
        )
        for node in range(5)
        for half in range(2)
    ]


def ghost_sums(place, slots, masters, weights, products, sends, back):
    spread = scatter(cell_entries(slots, products), OWN_ROWS, GHOST_ROWS)
    con_first = LOCAL_ROWS - OWN_ROWS
    for half in range(2):
        lanes = slice(128 * half, 128 * half + 128)
        sums = spread[con_first + half : con_first + half + 1, :]
        back[:, lanes] = weights[:, lanes] * jnp.broadcast_to(sums, (8, 128))
    spread = spread + scatter(con_entries(masters, back), OWN_ROWS, GHOST_ROWS)
    place_sends(
        place,
        -1,
        sends,
        lambda block: [spread[row : row + 1, :] for row in range(4 * block, 4 * block + 4)],
    )


def local_kernel(
    place_ref,
    received,
    relayed,
    cell_part,
    master_part,
    slots,
    scale,
    masters,
    weights,
    stiffness,
    products,
    sends,
    back,
    table,
    cell_values,
):
    place = place_ref[0]
    cell_products(
        place,
        received,
        relayed,
        cell_part,
        master_part,
        slots,
        scale,
        masters,
        weights,
        stiffness,
        table,
        cell_values,
        products,
    )
    ghost_sums(place, slots, masters, weights, products, sends, back)


def last_local_kernel(
    place_ref,
    received,
    relayed,
    cell_part,
    master_part,
    slots,
    scale,
    masters,
    weights,
    stiffness,
    reaction,
    first,
    second,
    third,
    products,
    sends,
    back,
    table,
    cell_values,
):
    local_kernel(
        place_ref,
        received,
        relayed,
        cell_part,
        master_part,
        slots,
        scale,
        masters,
        weights,
        stiffness,
        products,
        sends,
        back,
        table,
        cell_values,
    )
    vectors = [ref[...] for ref in (first, second, third)]
    sums = [jnp.sum(vectors[degree // 2] * vectors[(degree + 1) // 2]) for degree in range(5)]
    sums.append(
        jnp.sum(products[...] * cell_values[...])
        + jnp.sum(reaction[...] * vectors[2] * vectors[2])
    )
    lane = lax.broadcasted_iota(I32, (1, 128), 1)
    packed = jnp.zeros((1, 128), F32)
    for degree, value in enumerate(sums):
        packed = jnp.where(lane == degree, value, packed)
    for member in range(MEMBERS):
        sends[member, 4:5, :] = packed


def own_kernel(
    place_ref, slots, masters, products, back, reaction, vector, received, lists, own
):
    place = place_ref[0]
    entries = cell_entries(slots, products) + con_entries(masters, back)
    for block, offset in enumerate(OFFSETS):
        position = place + offset
        inside = (position >= 0) & (position < MEMBERS)
        member = lax.bitwise_and(position, MEMBERS - 1)
        for quarter in range(4):
            row = received[member, quarter : quarter + 1, :]
            entries.append(
                (
                    lists[block : block + 1, 128 * quarter : 128 * quarter + 128],
                    jnp.where(inside, row, 0.0),
                )
            )
    own[...] = scatter(entries, 0, OWN_ROWS) + reaction[...] * vector[...]


def owner_sum(place, own, relayed, lists, vector):
    entries = []
    back = place < 8
    for block in range(4):
        position = jnp.where(back, place - (block + 1), place + block + 1)
        outside = (position < 0) | (position >= MEMBERS)
        member = lax.bitwise_and(position, 3)
        for quarter in range(4):
            lanes = slice(128 * quarter, 128 * quarter + 128)
            slots = jnp.where(
                back, lists[block + 4 : block + 5, lanes], lists[block : block + 1, lanes]
            )
            row = relayed[member, quarter : quarter + 1, :]
            entries.append((slots, jnp.where(outside, row, 0.0)))
    vector[...] = own[...] + scatter(entries, 0, OWN_ROWS)


def owner_kernel(place_ref, own, relayed, lists, vector, sends):
    place = place_ref[0]
    owner_sum(place, own, relayed, lists, vector)
    pick_lists(place, vector, lists, sends)


def final_owner_kernel(place_ref, own, relayed, lists, vector):
    owner_sum(place_ref[0], own, relayed, lists, vector)


def group_kernel(received, sums):
    total = received[0, 4:5, :]
    for member in range(1, MEMBERS):
        total = total + received[member, 4:5, :]
    for member in range(sums.shape[0]):
        sums[member] = total


def last_kernel(moments, first, second, third, fourth, solution, residual):
    v = [ref[...] for ref in (first, second, third, fourth)]
    sums = moments[0]
    for member in range(1, moments.shape[0]):
        sums = sums + moments[member]
    lane = lax.broadcasted_iota(I32, (1, 128), 1)
    mu = [
        jnp.sum(jnp.where(lane == degree, sums, 0.0), axis=1, keepdims=True)
        for degree in range(6)
    ]
    zero = jnp.zeros((1, 1), F32)
    one = jnp.ones((1, 1), F32)

    def form(p, q, shift):
        value = zero
        for i, left in enumerate(p):
            for k, right in enumerate(q):
                value = value + left * right * mu[i + k + shift]
        return value

    res = [one]
    direction = [one]
    sol = [zero]
    rr = mu[0]
    for iteration in range(3):
        step = rr / form(direction, direction, 1)
        applied = [zero] + direction
        sol = [
            (sol[i] if i < len(sol) else zero) + step * direction[i]
            for i in range(len(direction))
        ]
        res = [
            (res[i] if i < len(res) else zero) - step * applied[i] for i in range(len(applied))
        ]
        if iteration < 2:
            rr_next = form(res, res, 0)
            ratio = rr_next / rr
            direction = [
                res[i] + (ratio * direction[i] if i < len(direction) else zero)
                for i in range(len(res))
            ]
            rr = rr_next
    solution[...] = sol[0] * v[0] + sol[1] * v[1] + sol[2] * v[2]
    residual[...] = res[0] * v[0] + res[1] * v[1] + res[2] * v[2] + res[3] * v[3]


def relay_pairs():
    pairs = []
    for group in range(32):
        for member in range(4):
            if group + 1 < 32:
                source = MEMBERS * group + member
                pairs.append((source, (source + MEMBERS) ^ 1))
            if group > 0:
                source = MEMBERS * group + 12 + member
                pairs.append((source, (source - MEMBERS) ^ 1))
    return pairs


def on_device(right_side, reaction, cell_slots, cell_level, con_masters, con_rows, send_lists):
    interp, stiffness = tables()
    place = lax.axis_index(GROUP).astype(I32)
    place_ref, relay_first = lax.optimization_barrier(
        (place.reshape(1), jnp.where(place < 4, 12, 0).astype(jnp.uint32))
    )
    whole = pl.BlockSpec(memory_space=pltpu.VMEM)
    scalar = pl.BlockSpec(memory_space=pltpu.SMEM)
    tile = jax.ShapeDtypeStruct((OWN_ROWS, 128), F32)
    sends = jax.ShapeDtypeStruct((MEMBERS, 4, 128), F32)
    vector = right_side.reshape(OWN_ROWS, 128)
    reaction = reaction.reshape(OWN_ROWS, 128)
    level = cell_level.reshape(1, 128)
    con_row = con_rows.reshape(1, 256)
    pairs = relay_pairs()

    def relay(received):
        rows = lax.dynamic_slice(
            received, (relay_first, np.uint32(0), np.uint32(0)), (4, 4, 128)
        )
        return lax.ppermute(rows, AXES, pairs)

    def kernel(body, outs, operands, scratch=(), ins_in_vmem=True, outs_in_vmem=True):
        in_vmem = [
            operand
            if operand is place_ref or not ins_in_vmem
            else pltpu.with_memory_space_constraint(operand, pltpu.VMEM)
            for operand in operands
        ]
        return pl.pallas_call(
            body,
            out_shape=jax.tree.map(lambda out: pltpu.VMEM(out.shape, out.dtype), outs)
            if outs_in_vmem
            else outs,
            in_specs=[scalar if operand is place_ref else whole for operand in operands],
            out_specs=jax.tree.map(lambda out: whole, outs),
            scratch_shapes=scratch,
        )(*in_vmem)

    padded = jax.ShapeDtypeStruct((128, 128), F32)
    con_padded = jax.ShapeDtypeStruct((8, 256), F32)
    work = [pltpu.VMEM((24, 128), F32), pltpu.VMEM((128, 128), F32)]
    packed, vector, slots, masters, weights, scale, stiffness, reaction = kernel(
        first_kernel,
        (
            sends,
            tile,
            jax.ShapeDtypeStruct((128, 128), I32),
            jax.ShapeDtypeStruct((8, 256), I32),
            con_padded,
            jax.ShapeDtypeStruct((1, 128), F32),
            padded,
            tile,
        ),
        (
            place_ref,
            vector,
            send_lists,
            cell_slots,
            con_masters,
            con_row,
            level,
            interp,
            stiffness,
            reaction,
        ),
        ins_in_vmem=False,
    )
    vectors = [vector]
    for step in range(3):
        vector = vectors[-1]
        received = lax.all_to_all(packed, GROUP, 0, 0)
        cell_part, master_part = kernel(
            near_kernel,
            (padded, con_padded),
            (place_ref, vector, received, slots, masters),
            [pltpu.VMEM((LOCAL_ROWS, 128), F32)],
        )
        relayed = relay(received)
        operands = (
            place_ref,
            received,
            relayed,
            cell_part,
            master_part,
            slots,
            scale,
            masters,
            weights,
            stiffness,
        )
        if step < 2:
            products, packed, back = kernel(
                local_kernel, (padded, sends, con_padded), operands, work
            )
        else:
            products, packed, back = kernel(
                last_local_kernel,
                (padded, jax.ShapeDtypeStruct((MEMBERS, 8, 128), F32), con_padded),
                operands + (reaction,) + tuple(vectors),
                work,
            )
        received = lax.all_to_all(packed, GROUP, 0, 0)
        own = kernel(
            own_kernel,
            tile,
            (place_ref, slots, masters, products, back, reaction, vector, received, send_lists),
        )
        relayed = relay(received)
        if step < 2:
            vector, packed = kernel(
                owner_kernel, (tile, sends), (place_ref, own, relayed, send_lists)
            )
            vectors.append(vector)
        else:
            sums = kernel(group_kernel, jax.ShapeDtypeStruct((32, 1, 128), F32), (received,))
            moments = lax.all_to_all(sums, REST, 0, 0)
            vector = kernel(final_owner_kernel, tile, (place_ref, own, relayed, send_lists))
            vectors.append(vector)
    solution_rows, residual_rows = kernel(
        last_kernel, (tile, tile), (moments, *vectors), outs_in_vmem=False
    )
    return (solution_rows.reshape(-1), residual_rows.reshape(-1))


def solution(mesh):
    torus = Mesh(mesh.devices.reshape(mesh.shape["gx"], 4, 8, 2), AXES)
    placed = (
        P(AXES),
        P(AXES),
        P(None, AXES),
        P(AXES),
        P(None, AXES),
        P(AXES),
        P(None, AXES),
    )
    return jax.shard_map(
        on_device, mesh=torus, in_specs=placed, out_specs=(P(AXES), P(AXES)), check_vma=False
    )
```

```python
import jax
import jax.numpy as jnp
import numpy as np
from jax import lax
from jax.experimental import pallas as pl
from jax.experimental.pallas import tpu as pltpu
from jax.sharding import Mesh
from jax.sharding import PartitionSpec as P

F32 = jnp.float32
BF16 = jnp.bfloat16
I32 = jnp.int32
AXES = ("gx", "gy_0", "gy_1", "gy_2")
GROUP = ("gy_1", "gy_2")
REST = ("gx", "gy_0")
OFFSETS = (1, 2, 3, 4, -1, -2, -3, -4)
MEMBERS = 16
PARTS = 3
OWN_ROWS = 64
LOCAL_ROWS = 96
GHOST_ROWS = 34


def lagrange(node_list, points):
    node_count = len(node_list)
    values = np.ones((len(points), node_count))
    derivs = np.zeros((len(points), node_count))
    for basis_node in range(node_count):
        for other_node in range(node_count):
            if other_node != basis_node:
                values[:, basis_node] = (
                    values[:, basis_node]
                    * (points - node_list[other_node])
                    / (node_list[basis_node] - node_list[other_node])
                )
        for skipped in range(node_count):
            if skipped != basis_node:
                product_term = np.ones(len(points)) / (node_list[basis_node] - node_list[skipped])
                for other_node in range(node_count):
                    if other_node != basis_node and other_node != skipped:
                        product_term = (
                            product_term
                            * (points - node_list[other_node])
                            / (node_list[basis_node] - node_list[other_node])
                        )
                derivs[:, basis_node] = derivs[:, basis_node] + product_term
    return (values, derivs)


def tables():
    gll_offset = np.sqrt(3.0 / 7.0)
    lobatto = np.array([0.0, (1.0 - gll_offset) / 2.0, 0.5, (1.0 + gll_offset) / 2.0, 1.0])
    inner_point = np.sqrt(5.0 - 2.0 * np.sqrt(10.0 / 7.0)) / 3.0
    outer_point = np.sqrt(5.0 + 2.0 * np.sqrt(10.0 / 7.0)) / 3.0
    inner_weight = (322.0 + 13.0 * np.sqrt(70.0)) / 900.0
    outer_weight = (322.0 - 13.0 * np.sqrt(70.0)) / 900.0
    points = np.array([-outer_point, -inner_point, 0.0, inner_point, outer_point])
    gauss_weights = np.array(
        [outer_weight, inner_weight, 128.0 / 225.0, inner_weight, outer_weight]
    )
    points = (points + 1.0) / 2.0
    gauss_weights = gauss_weights / 2.0
    shapes, slopes = lagrange(lobatto, points)
    fine_points = np.concatenate([lobatto / 2.0, (1.0 + lobatto) / 2.0])
    interp, _ = lagrange(lobatto, fine_points)
    quad_weights = np.kron(gauss_weights, np.kron(gauss_weights, gauss_weights))
    grad_x = np.kron(slopes, np.kron(shapes, shapes))
    grad_y = np.kron(shapes, np.kron(slopes, shapes))
    grad_z = np.kron(shapes, np.kron(shapes, slopes))
    stiffness = np.zeros((128, 128))
    for gradient in (grad_x, grad_y, grad_z):
        stiffness[:125, :125] += gradient.T @ (quad_weights[:, None] * gradient)
    interp_wide = np.zeros((8, 128))
    interp_wide[:5, :10] = interp.T
    return (jnp.asarray(interp_wide, F32), jnp.asarray(stiffness, F32))


def lane_pick(rows, lanes):
    return jnp.take_along_axis(rows, lanes, axis=1, mode="promise_in_bounds")


def pick(table, slots, first, last, picked=None, base=0):
    row_of = lax.shift_right_logical(slots, 7)
    lane_of = lax.bitwise_and(slots, 127)
    if picked is None:
        picked = jnp.zeros(slots.shape, F32)
    for row in range(first, last):
        spread_row = jnp.broadcast_to(table[row : row + 1, :], slots.shape)
        picked = jnp.where(row_of == base + row, lane_pick(spread_row, lane_of), picked)
    return picked


def split(x):
    pieces = []
    for part in range(PARTS):
        piece = x.astype(BF16)
        pieces.append(piece)
        if part + 1 < PARTS:
            x = x - piece.astype(F32)
    return pieces


def stacked(pieces, rows, tall):
    blocks = []
    for base in range(0, tall, 16):
        low = min(base // rows, PARTS - 1)
        high = min((base + 15) // rows, PARTS - 1)
        block = jnp.broadcast_to(pieces[low], (16, 128))
        if high > low:
            ids = lax.broadcasted_iota(I32, (16, 128), 0).astype(F32).astype(BF16)
            block = jnp.where(
                ids < jnp.full((16, 128), high * rows - base, BF16),
                block,
                jnp.broadcast_to(pieces[high], (16, 128)),
            )
        blocks.append(block)
    return jnp.concatenate(blocks, axis=0)


def scatter(entries, first, rows):
    tall = -(-PARTS * rows // 16) * 16
    row_ids = lax.broadcasted_iota(I32, (tall, 128), 0)
    row_ids = jnp.where(
        row_ids >= PARTS * rows,
        -256,
        row_ids - jnp.where(row_ids >= 2 * rows, 2 * rows, jnp.where(row_ids >= rows, rows, 0)),
    )
    row_ids = row_ids.astype(F32).astype(BF16)
    lane_ids = lax.broadcasted_iota(I32, (128, 128), 0).astype(F32).astype(BF16)
    none = jnp.zeros((tall, 128), BF16)
    total = None
    for start in range(0, len(entries), 16):
        row_values = []
        lane_hots = []
        for slots, values in entries[start : start + 16]:
            row_of = (lax.shift_right_logical(slots, 7) - first).astype(F32).astype(BF16)
            lane_of = lax.bitwise_and(slots, 127).astype(F32).astype(BF16)
            row_hot = row_ids == jnp.broadcast_to(row_of, (tall, 128))
            lane_hot = lane_ids == jnp.broadcast_to(lane_of, (128, 128))
            row_values.append(jnp.where(row_hot, stacked(split(values), rows, tall), none))
            lane_hots.append(
                jnp.where(lane_hot, jnp.ones((128, 128), BF16), jnp.zeros((128, 128), BF16))
            )
        part = lax.dot_general(
            jnp.concatenate(row_values, axis=1),
            jnp.concatenate(lane_hots, axis=1),
            (((1,), (1,)), ((), ())),
            preferred_element_type=F32,
        )
        total = part if total is None else total + part
    result = total[:rows, :]
    for part in range(1, PARTS):
        result = result + total[rows * part : rows * part + rows, :]
    return result


def place_sends(place, sign, sends, pull):
    for member in range(MEMBERS):
        sends[member] = jnp.zeros(sends.shape[1:], F32)
    for block, offset in enumerate(OFFSETS):
        position = place + sign * offset
        outside = (position < 0) | (position >= MEMBERS)
        member = lax.bitwise_xor(
            lax.bitwise_and(position, MEMBERS - 1), jnp.where(outside, 1, 0)
        )
        for quarter, row in enumerate(pull(block)):
            sends[member, quarter : quarter + 1, :] = row


def arrived(place, received, relayed, offset, quarter):
    position = place + offset
    member = lax.bitwise_and(position, MEMBERS - 1)
    outside = (position < 0) | (position >= MEMBERS)
    inner = received[member, quarter : quarter + 1, :]
    outer = relayed[lax.bitwise_and(member, 3), quarter : quarter + 1, :]
    return jnp.where(outside, outer, inner)


def pick_lists(place, vector, lists, sends):
    quarters = [
        pick(vector, lists[:, 128 * quarter : 128 * quarter + 128], 0, OWN_ROWS)
        for quarter in range(4)
    ]
    place_sends(
        place, 1, sends, lambda block: [quarter[block : block + 1, :] for quarter in quarters]
    )


def first_kernel(
    place_ref,
    vector_in,
    lists,
    slots_in,
    masters_in,
    con_row,
    level,
    interp,
    stiffness_in,
    reaction_in,
    sends,
    vector,
    slots,
    masters,
    weights,
    scale,
    stiffness,
    reaction,
):
    vector[...] = vector_in[...]
    pick_lists(place_ref[0], vector_in, lists, sends)
    slots[120:128, :] = jnp.zeros((8, 128), I32)
    slots[0:125, :] = slots_in[...]
    masters[...] = jnp.zeros((8, 256), I32)
    masters[0:5, :] = masters_in[...]
    for half in range(2):
        lanes = slice(128 * half, 128 * half + 128)
        weights[:, lanes] = lane_pick(
            interp[...], jnp.broadcast_to(con_row[:, lanes], (8, 128))
        )
    scale[...] = jnp.exp2(-level[...].astype(F32))
    one, two, three = split(stiffness_in[...])
    stiffness[...] = jnp.concatenate([one, two, three, one, two, one], axis=1)
    reaction[...] = reaction_in[...]


def near_kernel(place_ref, vector, received, slots, masters, cell_part, master_part, table):
    place = place_ref[0]
    table[0:OWN_ROWS, :] = vector[...]
    for block, offset in enumerate(OFFSETS):
        member = lax.bitwise_and(place - offset, MEMBERS - 1)
        for quarter in range(4):
            row = OWN_ROWS + 4 * block + quarter
            table[row : row + 1, :] = received[member, quarter : quarter + 1, :]
    for half in range(2):
        lanes = slice(128 * half, 128 * half + 128)
        master_part[:, lanes] = pick(table, masters[:, lanes], 0, LOCAL_ROWS)
    for group in range(16):
        group_rows = slice(8 * group, 8 * group + 8)
        cell_part[group_rows, :] = pick(table, slots[group_rows, :], 0, LOCAL_ROWS)


def cell_products(
    place,
    received,
    relayed,
    cell_part,
    master_part,
    slots,
    scale,
    masters,
    weights,
    stiffness,
    table,
    cell_values,
    products,
):
    forward = place < 8
    base = jnp.where(forward, OWN_ROWS, OWN_ROWS + 16)
    for block in range(4):
        offset = jnp.where(forward, block + 1, -(block + 1))
        for quarter in range(4):
            row = 4 * block + quarter
            table[row : row + 1, :] = arrived(place, received, relayed, -offset, quarter)
    for half in range(2):
        lanes = slice(128 * half, 128 * half + 128)
        resolved = weights[:, lanes] * pick(
            table, masters[:, lanes], 0, 16, master_part[:, lanes], base
        )
        table[16 + half : 17 + half, :] = jnp.sum(resolved, axis=0, keepdims=True)
    for group in range(16):
        group_rows = slice(8 * group, 8 * group + 8)
        at = slots[group_rows, :]
        values = pick(table, at, 0, 16, cell_part[group_rows, :], base)
        cell_values[group_rows, :] = pick(table, at, 16, 18, values, LOCAL_ROWS - 16)
    one, two, three = split(cell_values[...])
    products[...] = jnp.dot(
        stiffness[...],
        jnp.concatenate([three, two, one, two, one, one], axis=0),
        preferred_element_type=F32,
    ) * scale[...]


def cell_entries(slots, products):
    return [(slots[row : row + 1, :], products[row : row + 1, :]) for row in range(125)]


def con_entries(masters, back):
    return [
        (
            masters[node : node + 1, 128 * half : 128 * half + 128],
            back[node : node + 1, 128 * half : 128 * half + 128],
        )
        for node in range(5)
        for half in range(2)
    ]


def ghost_sums(place, slots, masters, weights, products, sends, back):
    spread = scatter(cell_entries(slots, products), OWN_ROWS, GHOST_ROWS)
    con_first = LOCAL_ROWS - OWN_ROWS
    for half in range(2):
        lanes = slice(128 * half, 128 * half + 128)
        sums = spread[con_first + half : con_first + half + 1, :]
        back[:, lanes] = weights[:, lanes] * jnp.broadcast_to(sums, (8, 128))
    spread = spread + scatter(con_entries(masters, back), OWN_ROWS, GHOST_ROWS)
    place_sends(
        place,
        -1,
        sends,
        lambda block: [spread[row : row + 1, :] for row in range(4 * block, 4 * block + 4)],
    )


def local_kernel(
    place_ref,
    received,
    relayed,
    cell_part,
    master_part,
    slots,
    scale,
    masters,
    weights,
    stiffness,
    products,
    sends,
    back,
    table,
    cell_values,
):
    place = place_ref[0]
    cell_products(
        place,
        received,
        relayed,
        cell_part,
        master_part,
        slots,
        scale,
        masters,
        weights,
        stiffness,
        table,
        cell_values,
        products,
    )
    ghost_sums(place, slots, masters, weights, products, sends, back)


def last_local_kernel(
    place_ref,
    received,
    relayed,
    cell_part,
    master_part,
    slots,
    scale,
    masters,
    weights,
    stiffness,
    reaction,
    first,
    second,
    third,
    products,
    sends,
    back,
    table,
    cell_values,
):
    local_kernel(
        place_ref,
        received,
        relayed,
        cell_part,
        master_part,
        slots,
        scale,
        masters,
        weights,
        stiffness,
        products,
        sends,
        back,
        table,
        cell_values,
    )
    vectors = [ref[...] for ref in (first, second, third)]
    sums = [jnp.sum(vectors[degree // 2] * vectors[(degree + 1) // 2]) for degree in range(5)]
    sums.append(
        jnp.sum(products[...] * cell_values[...])
        + jnp.sum(reaction[...] * vectors[2] * vectors[2])
    )
    lane = lax.broadcasted_iota(I32, (1, 128), 1)
    packed = jnp.zeros((1, 128), F32)
    for degree, value in enumerate(sums):
        packed = jnp.where(lane == degree, value, packed)
    for member in range(MEMBERS):
        sends[member, 4:5, :] = packed


def own_kernel(
    place_ref, slots, masters, products, back, reaction, vector, received, lists, own
):
    place = place_ref[0]
    entries = cell_entries(slots, products) + con_entries(masters, back)
    for block, offset in enumerate(OFFSETS):
        position = place + offset
        inside = (position >= 0) & (position < MEMBERS)
        member = lax.bitwise_and(position, MEMBERS - 1)
        for quarter in range(4):
            row = received[member, quarter : quarter + 1, :]
            entries.append(
                (
                    lists[block : block + 1, 128 * quarter : 128 * quarter + 128],
                    jnp.where(inside, row, 0.0),
                )
            )
    own[...] = scatter(entries, 0, OWN_ROWS) + reaction[...] * vector[...]


def owner_sum(place, own, relayed, lists, vector):
    entries = []
    back = place < 8
    for block in range(4):
        position = jnp.where(back, place - (block + 1), place + block + 1)
        outside = (position < 0) | (position >= MEMBERS)
        member = lax.bitwise_and(position, 3)
        for quarter in range(4):
            lanes = slice(128 * quarter, 128 * quarter + 128)
            slots = jnp.where(
                back, lists[block + 4 : block + 5, lanes], lists[block : block + 1, lanes]
            )
            row = relayed[member, quarter : quarter + 1, :]
            entries.append((slots, jnp.where(outside, row, 0.0)))
    vector[...] = own[...] + scatter(entries, 0, OWN_ROWS)


def owner_kernel(place_ref, own, relayed, lists, vector, sends):
    place = place_ref[0]
    owner_sum(place, own, relayed, lists, vector)
    pick_lists(place, vector, lists, sends)


def final_owner_kernel(place_ref, own, relayed, lists, vector):
    owner_sum(place_ref[0], own, relayed, lists, vector)


def group_kernel(received, sums):
    total = received[0, 4:5, :]
    for member in range(1, MEMBERS):
        total = total + received[member, 4:5, :]
    for member in range(sums.shape[0]):
        sums[member] = total


def last_kernel(moments, first, second, third, fourth, solution, residual):
    v = [ref[...] for ref in (first, second, third, fourth)]
    sums = moments[0]
    for member in range(1, moments.shape[0]):
        sums = sums + moments[member]
    lane = lax.broadcasted_iota(I32, (1, 128), 1)
    mu = [
        jnp.sum(jnp.where(lane == degree, sums, 0.0), axis=1, keepdims=True)
        for degree in range(6)
    ]
    zero = jnp.zeros((1, 1), F32)
    one = jnp.ones((1, 1), F32)

    def form(p, q, shift):
        value = zero
        for i, left in enumerate(p):
            for k, right in enumerate(q):
                value = value + left * right * mu[i + k + shift]
        return value

    res = [one]
    direction = [one]
    sol = [zero]
    rr = mu[0]
    for iteration in range(3):
        step = rr / form(direction, direction, 1)
        applied = [zero] + direction
        sol = [
            (sol[i] if i < len(sol) else zero) + step * direction[i]
            for i in range(len(direction))
        ]
        res = [
            (res[i] if i < len(res) else zero) - step * applied[i] for i in range(len(applied))
        ]
        if iteration < 2:
            rr_next = form(res, res, 0)
            ratio = rr_next / rr
            direction = [
                res[i] + (ratio * direction[i] if i < len(direction) else zero)
                for i in range(len(res))
            ]
            rr = rr_next
    solution[...] = sol[0] * v[0] + sol[1] * v[1] + sol[2] * v[2]
    residual[...] = res[0] * v[0] + res[1] * v[1] + res[2] * v[2] + res[3] * v[3]


def relay_pairs():
    pairs = []
    for group in range(32):
        for member in range(4):
            if group + 1 < 32:
                source = MEMBERS * group + member
                pairs.append((source, (source + MEMBERS) ^ 1))
            if group > 0:
                source = MEMBERS * group + 12 + member
                pairs.append((source, (source - MEMBERS) ^ 1))
    return pairs


def on_device(right_side, reaction, cell_slots, cell_level, con_masters, con_rows, send_lists):
    interp, stiffness = tables()
    place = lax.axis_index(GROUP).astype(I32)
    place_ref, relay_first = lax.optimization_barrier(
        (place.reshape(1), jnp.where(place < 4, 12, 0).astype(jnp.uint32))
    )
    whole = pl.BlockSpec(memory_space=pltpu.VMEM)
    scalar = pl.BlockSpec(memory_space=pltpu.SMEM)
    tile = jax.ShapeDtypeStruct((OWN_ROWS, 128), F32)
    sends = jax.ShapeDtypeStruct((MEMBERS, 4, 128), F32)
    vector = right_side.reshape(OWN_ROWS, 128)
    reaction = reaction.reshape(OWN_ROWS, 128)
    level = cell_level.reshape(1, 128)
    con_row = con_rows.reshape(1, 256)
    pairs = relay_pairs()

    def relay(received):
        rows = lax.dynamic_slice(
            received, (relay_first, np.uint32(0), np.uint32(0)), (4, 4, 128)
        )
        return lax.ppermute(rows, AXES, pairs)

    def kernel(body, outs, operands, scratch=(), ins_in_vmem=True, outs_in_vmem=True):
        in_vmem = [
            operand
            if operand is place_ref or not ins_in_vmem
            else pltpu.with_memory_space_constraint(operand, pltpu.VMEM)
            for operand in operands
        ]
        return pl.pallas_call(
            body,
            out_shape=jax.tree.map(lambda out: pltpu.VMEM(out.shape, out.dtype), outs)
            if outs_in_vmem
            else outs,
            in_specs=[scalar if operand is place_ref else whole for operand in operands],
            out_specs=jax.tree.map(lambda out: whole, outs),
            scratch_shapes=scratch,
        )(*in_vmem)

    padded = jax.ShapeDtypeStruct((128, 128), F32)
    con_padded = jax.ShapeDtypeStruct((8, 256), F32)
    work = [pltpu.VMEM((24, 128), F32), pltpu.VMEM((128, 128), F32)]
    packed, vector, slots, masters, weights, scale, stiffness, reaction = kernel(
        first_kernel,
        (
            sends,
            tile,
            jax.ShapeDtypeStruct((128, 128), I32),
            jax.ShapeDtypeStruct((8, 256), I32),
            con_padded,
            jax.ShapeDtypeStruct((1, 128), F32),
            jax.ShapeDtypeStruct((128, 768), BF16),
            tile,
        ),
        (
            place_ref,
            vector,
            send_lists,
            cell_slots,
            con_masters,
            con_row,
            level,
            interp,
            stiffness,
            reaction,
        ),
        ins_in_vmem=False,
    )
    vectors = [vector]
    for step in range(3):
        vector = vectors[-1]
        received = lax.all_to_all(packed, GROUP, 0, 0)
        cell_part, master_part = kernel(
            near_kernel,
            (padded, con_padded),
            (place_ref, vector, received, slots, masters),
            [pltpu.VMEM((LOCAL_ROWS, 128), F32)],
        )
        relayed = relay(received)
        operands = (
            place_ref,
            received,
            relayed,
            cell_part,
            master_part,
            slots,
            scale,
            masters,
            weights,
            stiffness,
        )
        if step < 2:
            products, packed, back = kernel(
                local_kernel, (padded, sends, con_padded), operands, work
            )
        else:
            products, packed, back = kernel(
                last_local_kernel,
                (padded, jax.ShapeDtypeStruct((MEMBERS, 8, 128), F32), con_padded),
                operands + (reaction,) + tuple(vectors),
                work,
            )
        received = lax.all_to_all(packed, GROUP, 0, 0)
        own = kernel(
            own_kernel,
            tile,
            (place_ref, slots, masters, products, back, reaction, vector, received, send_lists),
        )
        relayed = relay(received)
        if step < 2:
            vector, packed = kernel(
                owner_kernel, (tile, sends), (place_ref, own, relayed, send_lists)
            )
            vectors.append(vector)
        else:
            sums = kernel(group_kernel, jax.ShapeDtypeStruct((32, 1, 128), F32), (received,))
            moments = lax.all_to_all(sums, REST, 0, 0)
            vector = kernel(final_owner_kernel, tile, (place_ref, own, relayed, send_lists))
            vectors.append(vector)
    solution_rows, residual_rows = kernel(
        last_kernel, (tile, tile), (moments, *vectors), outs_in_vmem=False
    )
    return (solution_rows.reshape(-1), residual_rows.reshape(-1))


def solution(mesh):
    torus = Mesh(mesh.devices.reshape(mesh.shape["gx"], 4, 8, 2), AXES)
    placed = (
        P(AXES),
        P(AXES),
        P(None, AXES),
        P(AXES),
        P(None, AXES),
        P(AXES),
        P(None, AXES),
    )
    return jax.shard_map(
        on_device, mesh=torus, in_specs=placed, out_specs=(P(AXES), P(AXES)), check_vma=False
    )
```
